32 devices in a mesh: lat: 8 (over z, y), ch: 4 (over x, core).
Axes of the slice: x: 2, y: 2, z: 4, core: 2. Of those that a mesh axis runs over, the one named last changes fastest.
Arguments:
- state: float32 [1, 24, 180, 768], P(None, 'lat', None, 'ch'), may hold values from -30 to 30
- norm_gains: bfloat16 [2, 768], P(None, 'ch'), may hold values from 0.099609375 to 1.8984375
- channel_biases: bfloat16 [3, 768], P(None, 'ch'), may hold values from -2 to 2
- filter_in: float32 [2, 8, 96, 96], P(None, 'ch'), may hold values from -0.4375 to 0.4375
- filter_in_bias: float32 [2, 8, 96], P(None, 'ch'), may hold values from -2 to 2
- filter_out: float32 [2, 8, 96, 96], P(None, 'ch'), may hold values from -0.4375 to 0.4375
- filter_out_bias: float32 [2, 8, 96], P(None, 'ch'), may hold values from -2 to 2
- up_weight: bfloat16 [768, 3072], P(None, 'ch'), may hold values from -0.21875 to 0.21875
- up_bias: bfloat16 [3072], P('ch'), may hold values from -2 to 2
- down_weight: bfloat16 [3072, 768], P('ch'), may hold values from -0.109375 to 0.109375
Outputs:
- final_state: float32 [1, 24, 180, 768], P(None, 'lat', None, 'ch')
The draws below stay inside these ranges and needn't reach their ends.
All inputs are finite; a program needn't handle non-finite values.
Results may differ from the reference program's by a relative error of at most 0.0012.
Values may be sent and summed in bfloat16 or wider, within the bound.
A program may use at most 128 MiB of HBM per device.

```python
import math
import jax
import jax.numpy as jnp
from jax import lax

D = 768
FF = 3072
W = 180
NB = 8
M = 64
STEPS = 4
B = 1
H = 24
BS = 96


def draw_state(key, part):
    subkeys = jax.random.split(key, 3)
    channel_pos = jnp.arange(D).astype(jnp.float32) / D
    column_scale = 0.3 * jnp.exp(jax.random.uniform(subkeys[0], (D,), jnp.float32) * math.log(10.0)) * jnp.exp(channel_pos * 0.5 * math.log(3.0))
    channel_shift = 0.2 + 0.6 * channel_pos + 0.3 * jax.random.normal(subkeys[1], (D,), jnp.float32)
    value = jax.random.normal(subkeys[2], (B, H, W, D), jnp.float32) * column_scale + channel_shift
    return jnp.clip(value, -30.0, 30.0)


def block_scale(own_key, shape, cuts, smallest, high):
    level = 1.0
    for dim, shards_of in cuts:
        steps = jax.random.uniform(jax.random.fold_in(jax.random.fold_in(own_key, 6), dim), (shards_of,), jnp.float32, smallest / len(cuts), high / len(cuts))
        level = level * jnp.repeat(jnp.exp(steps), shape[dim] // shards_of).reshape((-1,) + (1,) * (len(shape) - 1 - dim))
    return level


def scatter_about(own_key, dims, scale, most, cuts=(), kind=jnp.bfloat16):
    values = scale * jax.random.normal(own_key, dims, jnp.float32)
    if cuts:
        values = values * block_scale(own_key, dims, cuts, -0.22, 0.18)
    return jnp.clip(values, -most, most).astype(kind)


def setup_inputs(seed: int = 0) -> dict:
    key_list = jax.random.split(jax.random.key(seed), 11)
    state = draw_state(jax.random.fold_in(key_list[10], 71), 0)
    norm_gains = jnp.clip(1.0 + 0.18 * jax.random.normal(key_list[1], (2, D), jnp.float32), 0.099609375, 1.8984375).astype(jnp.bfloat16)
    channel_biases = scatter_about(key_list[2], (3, D), 0.3, 2.0, ((1, 4),))
    filter_in = scatter_about(key_list[3], (2, NB, BS, BS), (2 * BS) ** -0.5, 0.4375, ((1, 4),), jnp.float32)
    filter_in_bias = scatter_about(key_list[4], (2, NB, BS), 0.3, 2.0, ((1, 4),), jnp.float32)
    filter_out = scatter_about(key_list[5], (2, NB, BS, BS), (2 * BS) ** -0.5, 0.4375, ((1, 4),), jnp.float32)
    filter_out_bias = scatter_about(key_list[6], (2, NB, BS), 0.3, 2.0, ((1, 4),), jnp.float32)
    up_weight = scatter_about(key_list[7], (D, FF), D ** -0.5, 0.21875, ((1, 4),))
    up_bias = scatter_about(key_list[8], (FF,), 0.3, 2.0, ((0, 4),))
    down_weight = scatter_about(key_list[9], (FF, D), FF ** -0.5, 0.109375, ((0, 4),))
    return dict(state=state, norm_gains=norm_gains, channel_biases=channel_biases, filter_in=filter_in, filter_in_bias=filter_in_bias, filter_out=filter_out, filter_out_bias=filter_out_bias, up_weight=up_weight, up_bias=up_bias, down_weight=down_weight)


EPS = 1e-05
SHRINK = 0.01
HIGH = lax.Precision.HIGHEST

def longitude_tables(width, modes):
    column = jnp.arange(width, dtype=jnp.int32)[:, None]
    order = jnp.arange(modes, dtype=jnp.int32)[None, :]
    angle = 2.0 * math.pi / width * (column * order % width).astype(jnp.float32)
    doubled = jnp.where(order == 0, 1.0, 2.0).astype(jnp.float32)
    return (jnp.cos(angle), jnp.sin(angle), jnp.cos(angle) * doubled, jnp.sin(angle) * doubled)

def latitude_tables(height):
    column = jnp.arange(height, dtype=jnp.int32)[:, None]
    order = jnp.arange(height, dtype=jnp.int32)[None, :]
    angle = 2.0 * math.pi / height * (column * order % height).astype(jnp.float32)
    return (jnp.cos(angle), jnp.sin(angle))

def layer_norm(values, gain, shift):
    mean = lax.optimization_barrier(jnp.sum(values, -1, keepdims=True)) / values.shape[-1]
    spread = lax.optimization_barrier(jnp.sum(values * values, -1, keepdims=True)) / values.shape[-1] - mean * mean
    return (values - mean) * lax.rsqrt(spread + EPS) * gain + shift

def soft_shrink(values):
    return jnp.where(values > SHRINK, values - SHRINK, jnp.where(values < -SHRINK, values + SHRINK, 0.0))

def block_apply(left, matrix):
    return jnp.einsum('bkmnj,nji->bkmni', left, matrix, precision=HIGH)

def spectral_mlp(real_part, imag_part, filter_in, filter_in_bias, filter_out, filter_out_bias):
    shape = real_part.shape
    blocks = filter_in.shape[1]
    size = filter_in.shape[2]
    real_blocks = real_part.reshape(shape[:-1] + (blocks, size))
    imag_blocks = imag_part.reshape(shape[:-1] + (blocks, size))
    first_real = jax.nn.relu(block_apply(real_blocks, filter_in[0]) - block_apply(imag_blocks, filter_in[1]) + filter_in_bias[0])
    first_imag = jax.nn.relu(block_apply(imag_blocks, filter_in[0]) + block_apply(real_blocks, filter_in[1]) + filter_in_bias[1])
    second_real = block_apply(first_real, filter_out[0]) - block_apply(first_imag, filter_out[1]) + filter_out_bias[0]
    second_imag = block_apply(first_imag, filter_out[0]) + block_apply(first_real, filter_out[1]) + filter_out_bias[1]
    return (soft_shrink(second_real).reshape(shape), soft_shrink(second_imag).reshape(shape))

def spectral_filter(normed, filter_in, filter_in_bias, filter_out, filter_out_bias):
    height = normed.shape[1]
    width = normed.shape[2]
    lon_cos, lon_sin, back_cos, back_sin = longitude_tables(width, M)
    lat_cos, lat_sin = latitude_tables(height)
    scale = 1.0 / math.sqrt(height * width)
    real_lon = jnp.einsum('bhwd,wm->bhmd', normed, lon_cos, precision=HIGH)
    imag_lon = -jnp.einsum('bhwd,wm->bhmd', normed, lon_sin, precision=HIGH)
    real_spec = (jnp.einsum('kh,bhmd->bkmd', lat_cos, real_lon, precision=HIGH) + jnp.einsum('kh,bhmd->bkmd', lat_sin, imag_lon, precision=HIGH)) * scale
    imag_spec = (jnp.einsum('kh,bhmd->bkmd', lat_cos, imag_lon, precision=HIGH) - jnp.einsum('kh,bhmd->bkmd', lat_sin, real_lon, precision=HIGH)) * scale
    out_real, out_imag = spectral_mlp(real_spec, imag_spec, filter_in, filter_in_bias, filter_out, filter_out_bias)
    real_rows = jnp.einsum('kh,bkmd->bhmd', lat_cos, out_real, precision=HIGH) - jnp.einsum('kh,bkmd->bhmd', lat_sin, out_imag, precision=HIGH)
    imag_rows = jnp.einsum('kh,bkmd->bhmd', lat_cos, out_imag, precision=HIGH) + jnp.einsum('kh,bkmd->bhmd', lat_sin, out_real, precision=HIGH)
    back = jnp.einsum('bhmd,wm->bhwd', real_rows, back_cos, precision=HIGH) - jnp.einsum('bhmd,wm->bhwd', imag_rows, back_sin, precision=HIGH)
    return back * scale

def reference(state, norm_gains, channel_biases, filter_in, filter_in_bias, filter_out, filter_out_bias, up_weight, up_bias, down_weight):
    gains = norm_gains.astype(jnp.float32)
    shifts = channel_biases.astype(jnp.float32)
    values = state
    for step_index in range(STEPS):
        normed = layer_norm(values, gains[0], shifts[0])
        values = values + spectral_filter(normed, filter_in, filter_in_bias, filter_out, filter_out_bias) + normed
        normed_two = layer_norm(values, gains[1], shifts[1]).astype(jnp.bfloat16)
        flat = normed_two.reshape(-1, normed_two.shape[-1])
        pre = jnp.dot(flat, up_weight, preferred_element_type=jnp.float32) + up_bias.astype(jnp.float32)
        hidden = jax.nn.gelu(pre, approximate=False).astype(jnp.bfloat16)
        mixed = jnp.dot(hidden, down_weight, preferred_element_type=jnp.float32) + shifts[2]
        values = values + mixed.reshape(values.shape)
    return values
```

```python
import functools
import math

import jax
import jax.numpy as jnp
from jax import lax
import numpy as np
from jax.experimental import pallas as pl
from jax.experimental.pallas import tpu as pltpu
from jax.sharding import PartitionSpec as P

D = 768
M = 64
STEPS = 4


EPS = 1e-05
SHRINK = 0.01
HIGH = lax.Precision.HIGHEST


def longitude_tables(width, modes):
    column = jnp.arange(width, dtype=jnp.int32)[:, None]
    order = jnp.arange(modes, dtype=jnp.int32)[None, :]
    angle = 2.0 * math.pi / width * (column * order % width).astype(jnp.float32)
    doubled = jnp.where(order == 0, 1.0, 2.0).astype(jnp.float32)
    return (jnp.cos(angle), jnp.sin(angle), jnp.cos(angle) * doubled, jnp.sin(angle) * doubled)


def latitude_tables(height):
    column = jnp.arange(height, dtype=jnp.int32)[:, None]
    order = jnp.arange(height, dtype=jnp.int32)[None, :]
    angle = 2.0 * math.pi / height * (column * order % height).astype(jnp.float32)
    return (jnp.cos(angle), jnp.sin(angle))


def layer_norm(values, gain, shift):
    mean = jnp.sum(values, -1, keepdims=True) / values.shape[-1]
    spread = jnp.sum(values * values, -1, keepdims=True) / values.shape[-1] - mean * mean
    return (values - mean) * lax.rsqrt(spread + EPS) * gain + shift


def soft_shrink(values):
    return jnp.where(
        values > SHRINK, values - SHRINK, jnp.where(values < -SHRINK, values + SHRINK, 0.0)
    )


def block_apply(left, matrix):
    return jnp.einsum("bkmnj,nji->bkmni", left, matrix, precision=HIGH)


def spectral_mlp(real_part, imag_part, filter_in, filter_in_bias, filter_out, filter_out_bias):
    shape = real_part.shape
    blocks = filter_in.shape[1]
    size = filter_in.shape[2]
    real_blocks = real_part.reshape(shape[:-1] + (blocks, size))
    imag_blocks = imag_part.reshape(shape[:-1] + (blocks, size))
    first_real = jax.nn.relu(
        block_apply(real_blocks, filter_in[0])
        - block_apply(imag_blocks, filter_in[1])
        + filter_in_bias[0]
    )
    first_imag = jax.nn.relu(
        block_apply(imag_blocks, filter_in[0])
        + block_apply(real_blocks, filter_in[1])
        + filter_in_bias[1]
    )
    second_real = (
        block_apply(first_real, filter_out[0])
        - block_apply(first_imag, filter_out[1])
        + filter_out_bias[0]
    )
    second_imag = (
        block_apply(first_imag, filter_out[0])
        + block_apply(first_real, filter_out[1])
        + filter_out_bias[1]
    )
    return (soft_shrink(second_real).reshape(shape), soft_shrink(second_imag).reshape(shape))


def local(
    state,
    norm_gains,
    channel_biases,
    filter_in,
    filter_in_bias,
    filter_out,
    filter_out_bias,
    up_weight,
    up_bias,
    down_weight,
):
    width = state.shape[2]
    height = state.shape[1] * lax.axis_size("lat")
    scale = 1.0 / math.sqrt(height * width)
    lon_cos, lon_sin, back_cos, back_sin = longitude_tables(width, M)
    lat_cos, lat_sin = latitude_tables(height)
    gains = norm_gains.astype(jnp.float32)
    shifts = channel_biases.astype(jnp.float32)
    full_up, full_gains, full_biases = (
        lax.all_gather(up_weight, "ch", axis=1, tiled=True),
        lax.all_gather(norm_gains, "ch", axis=1, tiled=True),
        lax.all_gather(channel_biases, "ch", axis=1, tiled=True),
    )
    full_down, full_up_bias = (
        lax.all_gather(down_weight, "ch", axis=0, tiled=True),
        lax.all_gather(up_bias, "ch", axis=0, tiled=True),
    )
    wide_gains = full_gains.astype(jnp.float32)
    wide_biases = full_biases.astype(jnp.float32)
    wide_up_bias = full_up_bias.astype(jnp.float32)
    values = state
    for step_index in range(STEPS):
        total, squares = lax.psum(
            (jnp.sum(values, -1, keepdims=True), jnp.sum(values * values, -1, keepdims=True)), "ch"
        )
        mean = total / D
        mean, spread = (mean, squares / D - mean * mean)
        normed = (values - mean) * lax.rsqrt(spread + EPS) * gains[0] + shifts[0]
        real_lon = jnp.einsum("bhwd,wm->bhmd", normed, lon_cos, precision=HIGH)
        imag_lon = -jnp.einsum("bhwd,wm->bhmd", normed, lon_sin, precision=HIGH)
        stacked = lax.all_to_all(
            jnp.stack((real_lon, imag_lon)), "lat", split_axis=3, concat_axis=2, tiled=True
        )
        spectral_real_lon = stacked[0]
        spectral_imag_lon = stacked[1]
        real_spec = (
            jnp.einsum("kh,bhmd->bkmd", lat_cos, spectral_real_lon, precision=HIGH)
            + jnp.einsum("kh,bhmd->bkmd", lat_sin, spectral_imag_lon, precision=HIGH)
        ) * scale
        imag_spec = (
            jnp.einsum("kh,bhmd->bkmd", lat_cos, spectral_imag_lon, precision=HIGH)
            - jnp.einsum("kh,bhmd->bkmd", lat_sin, spectral_real_lon, precision=HIGH)
        ) * scale
        out_real, out_imag = spectral_mlp(
            real_spec, imag_spec, filter_in, filter_in_bias, filter_out, filter_out_bias
        )
        real_rows = jnp.einsum("kh,bkmd->bhmd", lat_cos, out_real, precision=HIGH) - jnp.einsum(
            "kh,bkmd->bhmd", lat_sin, out_imag, precision=HIGH
        )
        imag_rows = jnp.einsum("kh,bkmd->bhmd", lat_cos, out_imag, precision=HIGH) + jnp.einsum(
            "kh,bkmd->bhmd", lat_sin, out_real, precision=HIGH
        )
        rows = lax.all_to_all(
            jnp.stack((real_rows, imag_rows)), "lat", split_axis=2, concat_axis=3, tiled=True
        )
        back = jnp.einsum("bhmd,wm->bhwd", rows[0], back_cos, precision=HIGH) - jnp.einsum(
            "bhmd,wm->bhwd", rows[1], back_sin, precision=HIGH
        )
        values = values + back * scale + normed
        owned = lax.all_to_all(values, "ch", split_axis=2, concat_axis=3, tiled=True)
        normed_two = layer_norm(owned, wide_gains[1], wide_biases[1]).astype(jnp.bfloat16)
        flat = normed_two.reshape(-1, normed_two.shape[-1])
        pre = jnp.dot(flat, full_up, preferred_element_type=jnp.float32) + wide_up_bias
        hidden = jax.nn.gelu(pre, approximate=False).astype(jnp.bfloat16)
        mixed = jnp.dot(hidden, full_down, preferred_element_type=jnp.float32) + wide_biases[2]
        values = values + lax.all_to_all(
            mixed.reshape(owned.shape), "ch", split_axis=3, concat_axis=2, tiled=True
        )
    return values


F32 = jnp.float32
BF16 = jnp.bfloat16
MESH = pl.DeviceIdType.MESH


def split_table(table):
    high = np.asarray(table, np.float32).astype(jnp.bfloat16)
    low = (table - high.astype(np.float64)).astype(np.float32).astype(jnp.bfloat16)
    return np.stack((high, low))


def fourier_tables(width, part, height, modes, owners):
    scale = 1.0 / math.sqrt(height * width)
    share = modes // owners
    rows = height // owners
    half = -(-width // 2)
    token = np.arange(width)
    place = token // half * part + token % half
    order = np.arange(modes).reshape(owners, share)
    angle = 2.0 * np.pi / width * (order[:, :, None] * token % width)
    forward = np.zeros((owners, 2, share, 2 * part))
    forward[:, 0, :, place] = np.moveaxis(np.cos(angle), -1, 0)
    forward[:, 1, :, place] = np.moveaxis(-np.sin(angle), -1, 0)
    doubled = np.where(order == 0, 1.0, 2.0)[:, None, :, None] * scale
    backward = (forward * doubled).reshape(2 * modes, 2 * part).T
    forward = forward.reshape(2 * modes, 2 * part)
    turns = np.arange(height)
    turn = 2.0 * np.pi / height * (turns[:, None] * turns[None, :] % height)
    cos, sin, eye = np.cos(turn), np.sin(turn), np.eye(share)
    mix = np.array([[cos, sin], [-sin, cos]])
    size = 2 * height * share
    lat = np.einsum("abkh,mn->akmhbn", mix, eye).reshape(size, size) * scale
    unmix = np.array([[cos, -sin], [sin, cos]])
    back = np.einsum("bahk,mn->hbmakn", unmix, eye)
    back = back.reshape((owners, rows) + back.shape[1:]).swapaxes(0, 1).reshape(size, size)
    return tuple(split_table(t) for t in (forward, lat, back, backward))


def dot(left, right):
    return jnp.dot(left, right, preferred_element_type=F32)


def halves(values):
    high = values.astype(BF16)
    return high, (values - high.astype(F32)).astype(BF16)


def dot3(left, right):
    return dot(left[0], right[0]) + dot(left[1], right[0]) + dot(left[0], right[1])


def gelu(values):
    return 0.5 * values * (1.0 + lax.erf(values * (1.0 / math.sqrt(2.0))))


def flip(index, bits):
    bit, moved = 1, index
    while bit <= bits:
        if bits & bit:
            moved = moved + bit - 2 * bit * lax.rem(lax.div(index, bit), 2)
        bit *= 2
    return moved


STAT, LON, ROW, STAT2, TOK, MIX, SETUP = range(7)


def rollout(
    lats,
    chans,
    state,
    gains,
    shifts,
    fin_bias,
    fout_bias,
    up_bias,
    fin_hbm,
    fout_hbm,
    up_hbm,
    down_hbm,
    t_lon_hbm,
    t_lat_hbm,
    t_rows_hbm,
    t_back_hbm,
    out,
    x,
    stat_send,
    stat_recv,
    lon_send,
    lon_recv,
    row_send,
    row_recv,
    tok_send,
    tok_recv,
    mix_full,
    mix_send,
    mix_pair,
    mix_recv,
    bias_send,
    bias_recv,
    fin_raw,
    fout_raw,
    fin,
    fout,
    fin_b,
    fout_b,
    up,
    down,
    up_recv,
    down_recv,
    t_lon,
    t_lat,
    t_rows,
    t_back,
    hidden,
    load_sem,
    send_sem,
    recv_sem,
):
    lat, ch = lax.axis_index("lat"), lax.axis_index("ch")
    core, chip = lax.rem(ch, 2), lax.div(ch, 2)
    chips = chans // 2
    rows, width, own = state.shape
    part = x.shape[2]
    near = -(-width // 2)
    wide = chans * own
    hid = up.shape[1]
    spread_modes = t_lon.shape[1]

    def chan(q):
        return 2 * lax.rem(chip + q // 2, chips) + (core if q % 2 == 0 else 1 - core)

    def half_of(q):
        return core if q % 2 == 0 else 1 - core

    lat_order = sorted(range(1, lats), reverse=True)
    ch_order = tuple(range(2, chans)) + (1,)

    loads = [
        pltpu.make_async_copy(source, target, load_sem.at[n])
        for n, (source, target) in enumerate(
            (
                (fin_hbm, fin_raw),
                (fout_hbm, fout_raw),
                (t_lon_hbm, t_lon),
                (t_lat_hbm, t_lat),
                (t_rows_hbm, t_rows),
                (t_back_hbm, t_back),
                (up_hbm, up),
                (down_hbm, down),
            )
        )
    ]
    for each in loads:
        each.start()

    barrier = pltpu.get_barrier_semaphore()
    for k in lat_order:
        pl.semaphore_signal(barrier, inc=1, device_id={"lat": flip(lat, k)}, device_id_type=MESH)
    for q in ch_order:
        pl.semaphore_signal(barrier, inc=1, device_id={"ch": chan(q)}, device_id_type=MESH)

    def copy(kind, r, k, source, target, device):
        return pltpu.make_async_remote_copy(
            src_ref=source,
            dst_ref=target,
            send_sem=send_sem.at[kind, r, k],
            recv_sem=recv_sem.at[kind, r, k],
            device_id=device,
            device_id_type=MESH,
        )

    def stat_copies(kind, r):
        n = kind // STAT2
        return [
            copy(kind, r, q, stat_send.at[n, r], stat_recv.at[n, r, ch], {"ch": chan(q)})
            for q in ch_order
        ]

    def lon_copies(r):
        return [
            copy(LON, r, k, lon_send.at[r, flip(lat, k)], lon_recv.at[lat, r], {"lat": flip(lat, k)})
            for k in lat_order
        ]

    def row_copies(r):
        return [
            copy(ROW, r, k, row_send.at[r, flip(lat, k)], row_recv.at[r, lat], {"lat": flip(lat, k)})
            for k in lat_order
        ]

    def tok_copies(r):
        return [
            copy(TOK, r, q, tok_send.at[r, half_of(q)], tok_recv.at[r, ch], {"ch": chan(q)})
            for q in ch_order
        ]

    def mix_copies(r):
        copies = [
            copy(MIX, r, q, mix_send.at[r, chan(q)], mix_recv.at[r, q // 2 - 1, core], {"ch": chan(q)})
            for q in range(2, chans)
        ]
        copies.append(copy(MIX, r, 1, mix_full.at[r, chan(1)], mix_pair.at[r], {"ch": chan(1)}))
        return copies

    def start(copies):
        for each in copies:
            each.start()

    def finish(copies):
        for each in copies:
            each.wait()

    gain = gains[...].astype(F32)
    shift = shifts[...].astype(F32)
    bias_send[...] = jnp.broadcast_to(up_bias[...].astype(F32), bias_send.shape)
    x[...] = jnp.zeros_like(x)
    for r in range(rows):
        x[r, 0, 0:near] = state[r, 0:near]
        x[r, 1, 0 : width - near] = state[r, near:width]
    ones = jnp.ones((8, own), BF16)
    which = lax.broadcasted_iota(jnp.int32, (8, 2 * part), 0)

    def row_sums(values):
        dims = (((1,), (1,)), ((), ()))
        high, low = halves(values)
        return lax.dot_general(
            ones, high, dims, preferred_element_type=F32
        ) + lax.dot_general(ones, low, dims, preferred_element_type=F32)

    def send_stats(kind, r):
        n = kind // STAT2
        values = x[r].reshape(2 * part, own)
        sums = jnp.where(which == 0, row_sums(values), row_sums(values * values))
        stat_send[n, r] = sums
        stat_recv[n, r, pl.ds(ch, 1)] = sums[None]
        start(stat_copies(kind, r))

    def take_stats(kind, r):
        n = kind // STAT2
        finish(stat_copies(kind, r))
        total = stat_recv[n, r, 0]
        for c in range(1, chans):
            total = total + stat_recv[n, r, c]
        mean = total[0:1] / wide
        scaled = lax.rsqrt(total[1:2] / wide - mean * mean + EPS)
        both = jnp.transpose(jnp.where(which == 0, mean, scaled))
        return both[:, 0:1], both[:, 1:2]

    pl.semaphore_wait(barrier, lats + chans - 2)
    for r in range(rows):
        send_stats(STAT, r)
    partner = {"ch": chan(1)}
    setup = [
        copy(SETUP, 0, 0, up_hbm, up_recv, partner),
        copy(SETUP, 0, 1, down_hbm, down_recv, partner),
        copy(SETUP, 0, 2, bias_send, bias_recv, partner),
    ]
    start(setup)
    loads[0].wait()
    loads[1].wait()
    blocks, size = fin_raw.shape[1], fin_raw.shape[2]
    line = lax.broadcasted_iota(jnp.int32, (size, own), 0)
    lane = lax.broadcasted_iota(jnp.int32, (size, own), 1)
    for raw, target, bias, bias_target in (
        (fin_raw, fin, fin_bias, fin_b),
        (fout_raw, fout, fout_bias, fout_b),
    ):
        placed = 0.0
        for n in range(blocks):
            shifted = jnp.where(lane == line + n * size, 1.0, 0.0)
            select = shifted.astype(BF16)
            for p in range(2):
                high, low = halves(raw[p, n])
                target[p, 0, n * size : (n + 1) * size] = dot(high, select).astype(BF16)
                target[p, 1, n * size : (n + 1) * size] = dot(low, select).astype(BF16)
            placed = placed + jnp.dot(
                bias[:, n, :], shifted, precision=HIGH, preferred_element_type=F32
            )
        bias_target[...] = placed
    for each in loads[2:6]:
        each.wait()

    def complex_apply(pair, weights, bias):
        split = pair.shape[0] // 2
        pair = halves(pair)
        one = dot3(pair, (weights[0, 0], weights[0, 1]))
        two = dot3(pair, (weights[1, 0], weights[1, 1]))
        return (
            one[:split] - two[split:] + bias[0:1, :],
            one[split:] + two[:split] + bias[1:2, :],
        )

    @pl.loop(0, STEPS)
    def _(index):
        for r in range(rows):
            mean, scaled = take_stats(STAT, r)
            now = x[r].reshape(2 * part, own)
            normed = (now - mean) * scaled * gain[0:1] + shift[0:1]
            x[r] = (now + normed).reshape(2, part, own)
            spectra = dot3((t_lon[0], t_lon[1]), halves(normed))
            lon_send[r] = spectra.astype(BF16).reshape(lats, spread_modes // lats, own)
            start(lon_copies(r))
            lon_recv[pl.ds(lat, 1), r] = lon_send[r, pl.ds(lat, 1)]
        for r in range(rows):
            finish(lon_copies(r))
        data = lon_recv[...].reshape(-1, own)
        spec = dot(t_lat[0], data) + dot(t_lat[1], data)
        real, imag = complex_apply(spec, fin, fin_b)
        pair = jnp.concatenate((jnp.maximum(real, 0.0), jnp.maximum(imag, 0.0)), 0)
        real, imag = complex_apply(pair, fout, fout_b)
        pair = halves(jnp.concatenate((soft_shrink(real), soft_shrink(imag)), 0))
        for r in range(rows):
            cut = slice(r * spread_modes, (r + 1) * spread_modes)
            back = dot3((t_rows[0, cut], t_rows[1, cut]), pair)
            row_send[r] = back.astype(BF16).reshape(lats, spread_modes // lats, own)
            start(row_copies(r))
            row_recv[r, pl.ds(lat, 1)] = row_send[r, pl.ds(lat, 1)]
        for r in range(rows):
            finish(row_copies(r))
            data = row_recv[r].reshape(-1, own)
            back = dot(t_back[0], data) + dot(t_back[1], data)
            x[r] = x[r] + back.reshape(2, part, own)
            send_stats(STAT2, r)
        for r in range(rows):
            mean, scaled = take_stats(STAT2, r)
            now = x[r].reshape(2 * part, own)
            normed = (now - mean) * scaled * gain[1:2] + shift[1:2]
            tok_send[r] = normed.astype(BF16).reshape(2, part, own)
            start(tok_copies(r))
            tok_recv[r, pl.ds(ch, 1)] = tok_send[r, pl.ds(core, 1)]

        @pl.when(index == 0)
        def _():
            loads[6].wait()
            loads[7].wait()
            finish(setup)

        for r in range(rows):
            finish(tok_copies(r))
            for s, (weight, bias) in enumerate(((up, bias_send), (up_recv, bias_recv))):
                for lo in range(0, hid, 256):
                    cut = slice(lo, lo + 256)
                    pre = bias[0:1, cut]
                    for c in range(chans):
                        pre = pre + dot(tok_recv[r, c], weight[c * own : (c + 1) * own, cut])
                    hidden[s, :, cut] = gelu(pre).astype(BF16)
            mixed = dot(hidden[0], down[...]) + dot(hidden[1], down_recv[...])
            for c in range(chans):
                piece = mixed[:, c * own : (c + 1) * own]
                mix_full[r, c] = piece
                mix_send[r, c] = piece.astype(BF16)
            start(mix_copies(r))
        for r in range(rows):
            finish(mix_copies(r))
            for h, piece in ((core, mix_full[r, pl.ds(ch, 1)]), (1 - core, mix_pair[r][None])):
                for n in range(chips - 1):
                    piece = piece + mix_recv[r, n, pl.ds(h, 1)].astype(F32)
                x[r, pl.ds(h, 1)] = x[r, pl.ds(h, 1)] + piece + shift[2:3]

            @pl.when(index < STEPS - 1)
            def _():
                send_stats(STAT, r)

    for r in range(rows):
        out[r, 0:near] = x[r, 0, 0:near]
        out[r, near:width] = x[r, 1, 0 : width - near]


def fused(
    lats,
    chans,
    state,
    norm_gains,
    channel_biases,
    filter_in,
    filter_in_bias,
    filter_out,
    filter_out_bias,
    up_weight,
    up_bias,
    down_weight,
):
    _, rows, width, own = state.shape
    part = -(--(-width // 2) // 16) * 16
    share = 2 * M // lats
    hid = up_weight.shape[1]
    tables = tuple(
        jnp.asarray(t) for t in fourier_tables(width, part, rows * lats, M, lats)
    )
    args = (
        state[0],
        norm_gains,
        channel_biases,
        filter_in_bias,
        filter_out_bias,
        up_bias.reshape(1, hid),
        filter_in,
        filter_out,
        up_weight,
        down_weight,
    ) + tables
    vmem = pl.BlockSpec(memory_space=pltpu.VMEM)
    hbm = pl.BlockSpec(memory_space=pltpu.HBM)
    spectrum = (rows, lats, share, own)
    peers = max(lats, chans)
    result = pl.pallas_call(
        functools.partial(rollout, lats, chans),
        out_shape=jax.ShapeDtypeStruct((rows, width, own), F32),
        in_specs=[vmem] * 6 + [hbm] * 8,
        out_specs=vmem,
        scratch_shapes=[
            pltpu.VMEM((rows, 2, part, own), F32),
            pltpu.VMEM((2, rows, 8, 2 * part), F32),
            pltpu.VMEM((2, rows, chans, 8, 2 * part), F32),
            pltpu.VMEM(spectrum, BF16),
            pltpu.VMEM((lats, rows, share, own), BF16),
            pltpu.VMEM(spectrum, BF16),
            pltpu.VMEM(spectrum, BF16),
            pltpu.VMEM((rows, 2, part, own), BF16),
            pltpu.VMEM((rows, chans, part, own), BF16),
            pltpu.VMEM((rows, chans, part, own), F32),
            pltpu.VMEM((rows, chans, part, own), BF16),
            pltpu.VMEM((rows, part, own), F32),
            pltpu.VMEM((rows, chans // 2 - 1, 2, part, own), BF16),
            pltpu.VMEM((8, hid), F32),
            pltpu.VMEM((8, hid), F32),
            pltpu.VMEM(filter_in.shape, F32),
            pltpu.VMEM(filter_out.shape, F32),
            pltpu.VMEM((2, 2, own, own), BF16),
            pltpu.VMEM((2, 2, own, own), BF16),
            pltpu.VMEM((2, own), F32),
            pltpu.VMEM((2, own), F32),
            pltpu.VMEM(up_weight.shape, BF16),
            pltpu.VMEM(down_weight.shape, BF16),
            pltpu.VMEM(up_weight.shape, BF16),
            pltpu.VMEM(down_weight.shape, BF16),
        ]
        + [pltpu.VMEM(t.shape, BF16) for t in tables]
        + [
            pltpu.VMEM((2, part, hid), BF16),
            pltpu.SemaphoreType.DMA((8,)),
            pltpu.SemaphoreType.DMA((7, rows, peers)),
            pltpu.SemaphoreType.DMA((7, rows, peers)),
        ],
        compiler_params=pltpu.CompilerParams(
            collective_id=0, has_side_effects=True, vmem_limit_bytes=48 * 1024 * 1024
        ),
    )(*args)
    return result[None]


def dispatch(sizes, *args):
    lats, chans = sizes["lat"], sizes["ch"]
    if 2 * M // lats % 16 == 0 and chans > 2 and chans % 2 == 0:
        return fused(lats, chans, *args)
    return local(*args)


def solution(mesh):
    placed = (
        P(None, "lat", None, "ch"),
        P(None, "ch"),
        P(None, "ch"),
        P(None, "ch", None, None),
        P(None, "ch", None),
        P(None, "ch", None, None),
        P(None, "ch", None),
        P(None, "ch"),
        P("ch"),
        P("ch", None),
    )
    return jax.shard_map(
        functools.partial(dispatch, dict(mesh.shape)), mesh=mesh, in_specs=placed, out_specs=P(None, "lat", None, "ch"), check_vma=False
    )
```

```python
import functools
import math

import jax
import jax.numpy as jnp
from jax import lax
import numpy as np
from jax.experimental import pallas as pl
from jax.experimental.pallas import tpu as pltpu
from jax.sharding import PartitionSpec as P

D = 768
M = 64
STEPS = 4


EPS = 1e-05
SHRINK = 0.01
HIGH = lax.Precision.HIGHEST


def longitude_tables(width, modes):
    column = jnp.arange(width, dtype=jnp.int32)[:, None]
    order = jnp.arange(modes, dtype=jnp.int32)[None, :]
    angle = 2.0 * math.pi / width * (column * order % width).astype(jnp.float32)
    doubled = jnp.where(order == 0, 1.0, 2.0).astype(jnp.float32)
    return (jnp.cos(angle), jnp.sin(angle), jnp.cos(angle) * doubled, jnp.sin(angle) * doubled)


def latitude_tables(height):
    column = jnp.arange(height, dtype=jnp.int32)[:, None]
    order = jnp.arange(height, dtype=jnp.int32)[None, :]
    angle = 2.0 * math.pi / height * (column * order % height).astype(jnp.float32)
    return (jnp.cos(angle), jnp.sin(angle))


def layer_norm(values, gain, shift):
    mean = jnp.sum(values, -1, keepdims=True) / values.shape[-1]
    spread = jnp.sum(values * values, -1, keepdims=True) / values.shape[-1] - mean * mean
    return (values - mean) * lax.rsqrt(spread + EPS) * gain + shift


def soft_shrink(values):
    return jnp.where(
        values > SHRINK, values - SHRINK, jnp.where(values < -SHRINK, values + SHRINK, 0.0)
    )


def block_apply(left, matrix):
    return jnp.einsum("bkmnj,nji->bkmni", left, matrix, precision=HIGH)


def spectral_mlp(real_part, imag_part, filter_in, filter_in_bias, filter_out, filter_out_bias):
    shape = real_part.shape
    blocks = filter_in.shape[1]
    size = filter_in.shape[2]
    real_blocks = real_part.reshape(shape[:-1] + (blocks, size))
    imag_blocks = imag_part.reshape(shape[:-1] + (blocks, size))
    first_real = jax.nn.relu(
        block_apply(real_blocks, filter_in[0])
        - block_apply(imag_blocks, filter_in[1])
        + filter_in_bias[0]
    )
    first_imag = jax.nn.relu(
        block_apply(imag_blocks, filter_in[0])
        + block_apply(real_blocks, filter_in[1])
        + filter_in_bias[1]
    )
    second_real = (
        block_apply(first_real, filter_out[0])
        - block_apply(first_imag, filter_out[1])
        + filter_out_bias[0]
    )
    second_imag = (
        block_apply(first_imag, filter_out[0])
        + block_apply(first_real, filter_out[1])
        + filter_out_bias[1]
    )
    return (soft_shrink(second_real).reshape(shape), soft_shrink(second_imag).reshape(shape))


def local(
    state,
    norm_gains,
    channel_biases,
    filter_in,
    filter_in_bias,
    filter_out,
    filter_out_bias,
    up_weight,
    up_bias,
    down_weight,
):
    width = state.shape[2]
    height = state.shape[1] * lax.axis_size("lat")
    scale = 1.0 / math.sqrt(height * width)
    lon_cos, lon_sin, back_cos, back_sin = longitude_tables(width, M)
    lat_cos, lat_sin = latitude_tables(height)
    gains = norm_gains.astype(jnp.float32)
    shifts = channel_biases.astype(jnp.float32)
    full_up, full_gains, full_biases = (
        lax.all_gather(up_weight, "ch", axis=1, tiled=True),
        lax.all_gather(norm_gains, "ch", axis=1, tiled=True),
        lax.all_gather(channel_biases, "ch", axis=1, tiled=True),
    )
    full_down, full_up_bias = (
        lax.all_gather(down_weight, "ch", axis=0, tiled=True),
        lax.all_gather(up_bias, "ch", axis=0, tiled=True),
    )
    wide_gains = full_gains.astype(jnp.float32)
    wide_biases = full_biases.astype(jnp.float32)
    wide_up_bias = full_up_bias.astype(jnp.float32)
    values = state
    for step_index in range(STEPS):
        total, squares = lax.psum(
            (jnp.sum(values, -1, keepdims=True), jnp.sum(values * values, -1, keepdims=True)), "ch"
        )
        mean = total / D
        mean, spread = (mean, squares / D - mean * mean)
        normed = (values - mean) * lax.rsqrt(spread + EPS) * gains[0] + shifts[0]
        real_lon = jnp.einsum("bhwd,wm->bhmd", normed, lon_cos, precision=HIGH)
        imag_lon = -jnp.einsum("bhwd,wm->bhmd", normed, lon_sin, precision=HIGH)
        stacked = lax.all_to_all(
            jnp.stack((real_lon, imag_lon)), "lat", split_axis=3, concat_axis=2, tiled=True
        )
        spectral_real_lon = stacked[0]
        spectral_imag_lon = stacked[1]
        real_spec = (
            jnp.einsum("kh,bhmd->bkmd", lat_cos, spectral_real_lon, precision=HIGH)
            + jnp.einsum("kh,bhmd->bkmd", lat_sin, spectral_imag_lon, precision=HIGH)
        ) * scale
        imag_spec = (
            jnp.einsum("kh,bhmd->bkmd", lat_cos, spectral_imag_lon, precision=HIGH)
            - jnp.einsum("kh,bhmd->bkmd", lat_sin, spectral_real_lon, precision=HIGH)
        ) * scale
        out_real, out_imag = spectral_mlp(
            real_spec, imag_spec, filter_in, filter_in_bias, filter_out, filter_out_bias
        )
        real_rows = jnp.einsum("kh,bkmd->bhmd", lat_cos, out_real, precision=HIGH) - jnp.einsum(
            "kh,bkmd->bhmd", lat_sin, out_imag, precision=HIGH
        )
        imag_rows = jnp.einsum("kh,bkmd->bhmd", lat_cos, out_imag, precision=HIGH) + jnp.einsum(
            "kh,bkmd->bhmd", lat_sin, out_real, precision=HIGH
        )
        rows = lax.all_to_all(
            jnp.stack((real_rows, imag_rows)), "lat", split_axis=2, concat_axis=3, tiled=True
        )
        back = jnp.einsum("bhmd,wm->bhwd", rows[0], back_cos, precision=HIGH) - jnp.einsum(
            "bhmd,wm->bhwd", rows[1], back_sin, precision=HIGH
        )
        values = values + back * scale + normed
        owned = lax.all_to_all(values, "ch", split_axis=2, concat_axis=3, tiled=True)
        normed_two = layer_norm(owned, wide_gains[1], wide_biases[1]).astype(jnp.bfloat16)
        flat = normed_two.reshape(-1, normed_two.shape[-1])
        pre = jnp.dot(flat, full_up, preferred_element_type=jnp.float32) + wide_up_bias
        hidden = jax.nn.gelu(pre, approximate=False).astype(jnp.bfloat16)
        mixed = jnp.dot(hidden, full_down, preferred_element_type=jnp.float32) + wide_biases[2]
        values = values + lax.all_to_all(
            mixed.reshape(owned.shape), "ch", split_axis=3, concat_axis=2, tiled=True
        )
    return values


F32 = jnp.float32
BF16 = jnp.bfloat16
MESH = pl.DeviceIdType.MESH


def split_table(table):
    high = np.asarray(table, np.float32).astype(jnp.bfloat16)
    low = (table - high.astype(np.float64)).astype(np.float32).astype(jnp.bfloat16)
    return np.stack((high, low))


def fourier_tables(width, part, height, modes, owners):
    scale = 1.0 / math.sqrt(height * width)
    share = modes // owners
    rows = height // owners
    half = -(-width // 2)
    token = np.arange(width)
    place = token // half * part + token % half
    order = np.arange(modes).reshape(owners, share)
    angle = 2.0 * np.pi / width * (order[:, :, None] * token % width)
    forward = np.zeros((owners, 2, share, 2 * part))
    forward[:, 0, :, place] = np.moveaxis(np.cos(angle), -1, 0)
    forward[:, 1, :, place] = np.moveaxis(-np.sin(angle), -1, 0)
    doubled = np.where(order == 0, 1.0, 2.0)[:, None, :, None] * scale
    backward = (forward * doubled).reshape(2 * modes, 2 * part).T
    forward = forward.reshape(2 * modes, 2 * part)
    turns = np.arange(height)
    turn = 2.0 * np.pi / height * (turns[:, None] * turns[None, :] % height)
    cos, sin, eye = np.cos(turn), np.sin(turn), np.eye(share)
    mix = np.array([[cos, sin], [-sin, cos]])
    size = 2 * height * share
    lat = np.einsum("abkh,mn->akmhbn", mix, eye).reshape(size, size) * scale
    unmix = np.array([[cos, -sin], [sin, cos]])
    back = np.einsum("bahk,mn->hbmakn", unmix, eye)
    back = back.reshape((owners, rows) + back.shape[1:]).swapaxes(0, 1).reshape(size, size)
    return tuple(split_table(t) for t in (forward, lat, back, backward))


def dot(left, right):
    return jnp.dot(left, right, preferred_element_type=F32)


def halves(values):
    high = values.astype(BF16)
    return high, (values - high.astype(F32)).astype(BF16)


def dot3(left, right):
    return dot(left[0], right[0]) + dot(left[1], right[0]) + dot(left[0], right[1])


def gelu(values):
    return 0.5 * values * (1.0 + lax.erf(values * (1.0 / math.sqrt(2.0))))


def flip(index, bits):
    bit, moved = 1, index
    while bit <= bits:
        if bits & bit:
            moved = moved + bit - 2 * bit * lax.rem(lax.div(index, bit), 2)
        bit *= 2
    return moved


LANES = 128


def pack(values):
    rows = values.shape[-2] // 2
    rest = values[..., LANES:]
    folded = jnp.concatenate((rest[..., :rows, :], rest[..., rows:, :]), -1)
    return values[..., :LANES].astype(BF16), folded.astype(BF16)


def unfold(folded):
    values = folded.astype(F32)
    return jnp.concatenate((values[..., : LANES // 2], values[..., LANES // 2 :]), -2)


def store_packed(target, where, values):
    rows = values.shape[-2]
    full, folded = pack(values)
    target[where + (slice(0, rows),)] = full
    target[where + (slice(rows, rows + rows // 2),)] = folded


STAT, LON, ROW, STAT2, TOK, MIX, SETUP = range(7)


def rollout(
    lats,
    chans,
    state,
    gains,
    shifts,
    fin_bias,
    fout_bias,
    up_bias,
    fin_hbm,
    fout_hbm,
    up_hbm,
    down_hbm,
    t_lon_hbm,
    t_lat_hbm,
    t_rows_hbm,
    t_back_hbm,
    out,
    x,
    stat_send,
    stat_recv,
    lon_send,
    lon_recv,
    row_send,
    row_recv,
    tok_send,
    tok_recv,
    mix_full,
    mix_send,
    mix_pair,
    mix_recv,
    bias_send,
    bias_recv,
    fin_raw,
    fout_raw,
    fin,
    fout,
    fin_b,
    fout_b,
    up,
    down,
    up_recv,
    down_recv,
    t_lon,
    t_lat,
    t_rows,
    t_back,
    tokens,
    hidden,
    load_sem,
    send_sem,
    recv_sem,
):
    lat, ch = lax.axis_index("lat"), lax.axis_index("ch")
    core, chip = lax.rem(ch, 2), lax.div(ch, 2)
    chips = chans // 2
    rows, width, own = state.shape
    part = x.shape[2]
    near = -(-width // 2)
    wide = chans * own
    hid = up.shape[1]
    spread_modes = t_lon.shape[1]

    def chan(q):
        return 2 * lax.rem(chip + q // 2, chips) + (core if q % 2 == 0 else 1 - core)

    def half_of(q):
        return core if q % 2 == 0 else 1 - core

    up_rows = []
    for c in range(chans):
        up_rows.append((pl.ds(c * own, LANES), pl.ds(c * LANES, LANES)))
        rest = own - LANES
        up_rows.append((pl.ds(c * own + LANES, rest), pl.ds(chans * LANES + c * rest, rest)))

    lat_order = sorted(range(1, lats), reverse=True)
    ch_order = tuple(range(2, chans)) + (1,)

    loads = [
        pltpu.make_async_copy(source, target, load_sem.at[n])
        for n, (source, target) in enumerate(
            (
                (fin_hbm, fin_raw),
                (fout_hbm, fout_raw),
                (t_lon_hbm, t_lon),
                (t_lat_hbm, t_lat),
                (t_rows_hbm, t_rows),
                (t_back_hbm, t_back),
                (down_hbm, down),
            )
            + tuple((up_hbm.at[source], up.at[target]) for source, target in up_rows)
        )
    ]
    for each in loads:
        each.start()

    barrier = pltpu.get_barrier_semaphore()
    for k in lat_order:
        pl.semaphore_signal(barrier, inc=1, device_id={"lat": flip(lat, k)}, device_id_type=MESH)
    for q in ch_order:
        pl.semaphore_signal(barrier, inc=1, device_id={"ch": chan(q)}, device_id_type=MESH)

    def copy(kind, r, k, source, target, device):
        return pltpu.make_async_remote_copy(
            src_ref=source,
            dst_ref=target,
            send_sem=send_sem.at[kind, r, k],
            recv_sem=recv_sem.at[kind, r, k],
            device_id=device,
            device_id_type=MESH,
        )

    def stat_copies(kind, r):
        n = kind // STAT2
        return [
            copy(kind, r, q, stat_send.at[n, r], stat_recv.at[n, r, ch], {"ch": chan(q)})
            for q in ch_order
        ]

    def lon_copies(r):
        return [
            copy(LON, r, k, lon_send.at[r, flip(lat, k)], lon_recv.at[lat, r], {"lat": flip(lat, k)})
            for k in lat_order
        ]

    def row_copies(r):
        return [
            copy(ROW, r, k, row_send.at[r, flip(lat, k)], row_recv.at[r, lat], {"lat": flip(lat, k)})
            for k in lat_order
        ]

    def tok_copies(r):
        return [
            copy(TOK, r, q, tok_send.at[r, half_of(q)], tok_recv.at[r, ch], {"ch": chan(q)})
            for q in ch_order
        ]

    def mix_copies(r):
        copies = [
            copy(MIX, r, q, mix_send.at[r, chan(q)], mix_recv.at[r, q // 2 - 1, core], {"ch": chan(q)})
            for q in range(2, chans)
        ]
        copies.append(copy(MIX, r, 1, mix_full.at[r, chan(1)], mix_pair.at[r], {"ch": chan(1)}))
        return copies

    def start(copies):
        for each in copies:
            each.start()

    def finish(copies):
        for each in copies:
            each.wait()

    gain = gains[...].astype(F32)
    shift = shifts[...].astype(F32)
    bias_send[...] = jnp.broadcast_to(up_bias[...].astype(F32), bias_send.shape)
    x[...] = jnp.zeros_like(x)
    for r in range(rows):
        x[r, 0, 0:near] = state[r, 0:near]
        x[r, 1, 0 : width - near] = state[r, near:width]
    ones = jnp.ones((8, own), BF16)
    which = lax.broadcasted_iota(jnp.int32, (8, 2 * part), 0)

    def row_sums(values):
        dims = (((1,), (1,)), ((), ()))
        high, low = halves(values)
        return lax.dot_general(
            ones, high, dims, preferred_element_type=F32
        ) + lax.dot_general(ones, low, dims, preferred_element_type=F32)

    def send_stats(kind, r):
        n = kind // STAT2
        values = x[r].reshape(2 * part, own)
        sums = jnp.where(which == 0, row_sums(values), row_sums(values * values))
        stat_send[n, r] = sums
        stat_recv[n, r, pl.ds(ch, 1)] = sums[None]
        start(stat_copies(kind, r))

    def take_stats(kind, r):
        n = kind // STAT2
        with jax.named_scope(f"wait_stat#n={n}"):
            finish(stat_copies(kind, r))
        total = stat_recv[n, r, 0]
        for c in range(1, chans):
            total = total + stat_recv[n, r, c]
        mean = total[0:1] / wide
        scaled = lax.rsqrt(total[1:2] / wide - mean * mean + EPS)
        both = jnp.transpose(jnp.where(which == 0, mean, scaled))
        return both[:, 0:1], both[:, 1:2]

    pl.semaphore_wait(barrier, lats + chans - 2)
    for r in range(rows):
        send_stats(STAT, r)
    partner = {"ch": chan(1)}
    setup = [
        copy(SETUP, 0, 0, down_hbm, down_recv, partner),
        copy(SETUP, 0, 1, bias_send, bias_recv, partner),
    ]
    for n, (source, target) in enumerate(up_rows):
        setup.append(
            copy(SETUP, 1 + n // chans, n % chans, up_hbm.at[source], up_recv.at[target], partner)
        )
    start(setup)
    loads[0].wait()
    loads[1].wait()
    blocks, size = fin_raw.shape[1], fin_raw.shape[2]
    line = lax.broadcasted_iota(jnp.int32, (size, own), 0)
    lane = lax.broadcasted_iota(jnp.int32, (size, own), 1)
    for raw, target, bias, bias_target in (
        (fin_raw, fin, fin_bias, fin_b),
        (fout_raw, fout, fout_bias, fout_b),
    ):
        placed = 0.0
        for n in range(blocks):
            shifted = jnp.where(lane == line + n * size, 1.0, 0.0)
            select = shifted.astype(BF16)
            for p in range(2):
                high, low = halves(raw[p, n])
                target[p, 0, n * size : (n + 1) * size] = dot(high, select).astype(BF16)
                target[p, 1, n * size : (n + 1) * size] = dot(low, select).astype(BF16)
            placed = placed + jnp.dot(
                bias[:, n, :], shifted, precision=HIGH, preferred_element_type=F32
            )
        bias_target[...] = placed
    for each in loads[2:6]:
        each.wait()

    def complex_apply(pair, weights, bias):
        split = pair.shape[0] // 2
        pair = halves(pair)
        one = dot3(pair, (weights[0, 0], weights[0, 1]))
        two = dot3(pair, (weights[1, 0], weights[1, 1]))
        return (
            one[:split] - two[split:] + bias[0:1, :],
            one[split:] + two[:split] + bias[1:2, :],
        )

    def spectrum(messages, count):
        full = messages[..., :count, :]
        rest = unfold(messages[..., count:, :]).astype(BF16)
        return jnp.concatenate((full, rest), -1).reshape(-1, own)

    share = spread_modes // lats

    def forward(r):
        with jax.named_scope("forward"):
            mean, scaled = take_stats(STAT, r)
            now = x[r].reshape(2 * part, own)
            normed = (now - mean) * scaled * gain[0:1] + shift[0:1]
            x[r] = (now + normed).reshape(2, part, own)
            spectra = dot3((t_lon[0], t_lon[1]), halves(normed))
            store_packed(lon_send, (r, slice(None)), spectra.reshape(lats, share, own))
            start(lon_copies(r))
            lon_recv[pl.ds(lat, 1), r] = lon_send[r, pl.ds(lat, 1)]

    def spectral():
        data = spectrum(lon_recv[...], share)
        spec = dot(t_lat[0], data) + dot(t_lat[1], data)
        real, imag = complex_apply(spec, fin, fin_b)
        pair = jnp.concatenate((jnp.maximum(real, 0.0), jnp.maximum(imag, 0.0)), 0)
        real, imag = complex_apply(pair, fout, fout_b)
        return halves(jnp.concatenate((soft_shrink(real), soft_shrink(imag)), 0))

    def unmix(r, pair):
        cut = slice(r * spread_modes, (r + 1) * spread_modes)
        back = dot3((t_rows[0, cut], t_rows[1, cut]), pair)
        store_packed(row_send, (r, slice(None)), back.reshape(lats, share, own))
        start(row_copies(r))
        row_recv[r, pl.ds(lat, 1)] = row_send[r, pl.ds(lat, 1)]

    def backward(r):
        data = spectrum(row_recv[r], share)
        back = dot(t_back[0], data) + dot(t_back[1], data)
        x[r] = x[r] + back.reshape(2, part, own)
        send_stats(STAT2, r)

    def token(r):
        mean, scaled = take_stats(STAT2, r)
        now = x[r].reshape(2 * part, own)
        normed = (now - mean) * scaled * gain[1:2] + shift[1:2]
        store_packed(tok_send, (r, slice(None)), normed.reshape(2, part, own))
        start(tok_copies(r))
        tok_recv[r, pl.ds(ch, 1)] = tok_send[r, pl.ds(core, 1)]

    def project_up(r):
        for c in range(chans):
            tokens[:, c * LANES : (c + 1) * LANES] = tok_recv[r, c, 0:part]
        middle = part // 2
        for c in range(0, chans, 2):
            cut = slice((chans + c // 2) * LANES, (chans + c // 2 + 1) * LANES)
            one = tok_recv[r, c, part : part + middle]
            two = tok_recv[r, c + 1, part : part + middle]
            for n, lanes in enumerate((slice(0, LANES // 2), slice(LANES // 2, LANES))):
                pair = jnp.concatenate((one[:, lanes], two[:, lanes]), -1)
                tokens[n * middle : (n + 1) * middle, cut] = pair
        for s, (weight, bias) in enumerate(((up, bias_send), (up_recv, bias_recv))):
            for lo in range(0, hid, 256):
                cut = slice(lo, lo + 256)
                pre = dot(tokens[...], weight[:, cut]) + bias[0:1, cut]
                hidden[s, :, cut] = gelu(pre).astype(BF16)

    def project_down(r):
        mixed = dot(hidden[0], down[...]) + dot(hidden[1], down_recv[...])
        for c in range(chans):
            piece = mixed[:, c * own : (c + 1) * own]
            mix_full[r, c] = piece
            store_packed(mix_send, (r, c), piece)
        start(mix_copies(r))

    def residual(r):
        for h, piece in ((core, mix_full[r, pl.ds(ch, 1)]), (1 - core, mix_pair[r][None])):
            for n in range(chips - 1):
                message = mix_recv[r, n, pl.ds(h, 1)]
                rest = unfold(message[:, part:])
                piece = piece + jnp.concatenate((message[:, :part].astype(F32), rest), -1)
            x[r, pl.ds(h, 1)] = x[r, pl.ds(h, 1)] + piece + shift[2:3]

    forward(0)

    @pl.loop(0, STEPS)
    def _(index):
        for r in range(1, rows):
            forward(r)
        with jax.named_scope("wait_lon"):
            for r in range(rows):
                finish(lon_copies(r))
        with jax.named_scope("spectral"):
            pair = spectral()
        with jax.named_scope("unmix"):
            for r in range(rows):
                unmix(r, pair)
        for r in range(rows):
            with jax.named_scope("wait_row"):
                finish(row_copies(r))
            with jax.named_scope("backward"):
                backward(r)
        for r in range(rows):
            with jax.named_scope("token"):
                token(r)

        @pl.when(index == 0)
        def _():
            for each in loads[6:]:
                each.wait()
            finish(setup)

        for r in range(rows):
            with jax.named_scope("wait_tok"):
                finish(tok_copies(r))
            with jax.named_scope("up"):
                project_up(r)
            with jax.named_scope("down"):
                project_down(r)
        for r in range(rows):
            if r == rows - 1:

                @pl.when(index < STEPS - 1)
                def _():
                    forward(0)

            with jax.named_scope("wait_mix"):
                finish(mix_copies(r))
            with jax.named_scope("residual"):
                residual(r)

            @pl.when(index < STEPS - 1)
            def _():
                send_stats(STAT, r)

    for r in range(rows):
        out[r, 0:near] = x[r, 0, 0:near]
        out[r, near:width] = x[r, 1, 0 : width - near]


def fused(
    lats,
    chans,
    state,
    norm_gains,
    channel_biases,
    filter_in,
    filter_in_bias,
    filter_out,
    filter_out_bias,
    up_weight,
    up_bias,
    down_weight,
):
    _, rows, width, own = state.shape
    part = -(--(-width // 2) // 16) * 16
    share = 2 * M // lats
    hid = up_weight.shape[1]
    tables = tuple(
        jnp.asarray(t) for t in fourier_tables(width, part, rows * lats, M, lats)
    )
    args = (
        state[0],
        norm_gains,
        channel_biases,
        filter_in_bias,
        filter_out_bias,
        up_bias.reshape(1, hid),
        filter_in,
        filter_out,
        up_weight,
        down_weight,
    ) + tables
    vmem = pl.BlockSpec(memory_space=pltpu.VMEM)
    hbm = pl.BlockSpec(memory_space=pltpu.HBM)
    packed = share + share // 2
    spectrum = (rows, lats, packed, LANES)
    folded = part + part // 2
    peers = max(lats, chans)
    result = pl.pallas_call(
        functools.partial(rollout, lats, chans),
        out_shape=jax.ShapeDtypeStruct((rows, width, own), F32),
        in_specs=[vmem] * 6 + [hbm] * 8,
        out_specs=vmem,
        scratch_shapes=[
            pltpu.VMEM((rows, 2, part, own), F32),
            pltpu.VMEM((2, rows, 8, 2 * part), F32),
            pltpu.VMEM((2, rows, chans, 8, 2 * part), F32),
            pltpu.VMEM(spectrum, BF16),
            pltpu.VMEM((lats, rows, packed, LANES), BF16),
            pltpu.VMEM(spectrum, BF16),
            pltpu.VMEM(spectrum, BF16),
            pltpu.VMEM((rows, 2, folded, LANES), BF16),
            pltpu.VMEM((rows, chans, folded, LANES), BF16),
            pltpu.VMEM((rows, chans, part, own), F32),
            pltpu.VMEM((rows, chans, folded, LANES), BF16),
            pltpu.VMEM((rows, part, own), F32),
            pltpu.VMEM((rows, chans // 2 - 1, 2, folded, LANES), BF16),
            pltpu.VMEM((8, hid), F32),
            pltpu.VMEM((8, hid), F32),
            pltpu.VMEM(filter_in.shape, F32),
            pltpu.VMEM(filter_out.shape, F32),
            pltpu.VMEM((2, 2, own, own), BF16),
            pltpu.VMEM((2, 2, own, own), BF16),
            pltpu.VMEM((2, own), F32),
            pltpu.VMEM((2, own), F32),
            pltpu.VMEM(up_weight.shape, BF16),
            pltpu.VMEM(down_weight.shape, BF16),
            pltpu.VMEM(up_weight.shape, BF16),
            pltpu.VMEM(down_weight.shape, BF16),
        ]
        + [pltpu.VMEM(t.shape, BF16) for t in tables]
        + [
            pltpu.VMEM((part, chans * own), BF16),
            pltpu.VMEM((2, part, hid), BF16),
            pltpu.SemaphoreType.DMA((7 + 2 * chans,)),
            pltpu.SemaphoreType.DMA((7, rows, peers)),
            pltpu.SemaphoreType.DMA((7, rows, peers)),
        ],
        compiler_params=pltpu.CompilerParams(
            collective_id=0, has_side_effects=True, vmem_limit_bytes=60 * 1024 * 1024
        ),
    )(*args)
    return result[None]


def dispatch(sizes, *args):
    lats, chans = sizes["lat"], sizes["ch"]
    own = args[0].shape[3]
    folds = own // LANES == 1 and 2 * (own % LANES) == LANES
    if folds and 2 * M // lats % 16 == 0 and chans > 2 and chans % 2 == 0:
        return fused(lats, chans, *args)
    return local(*args)


def solution(mesh):
    placed = (
        P(None, "lat", None, "ch"),
        P(None, "ch"),
        P(None, "ch"),
        P(None, "ch", None, None),
        P(None, "ch", None),
        P(None, "ch", None, None),
        P(None, "ch", None),
        P(None, "ch"),
        P("ch"),
        P("ch", None),
    )
    return jax.shard_map(
        functools.partial(dispatch, dict(mesh.shape)), mesh=mesh, in_specs=placed, out_specs=P(None, "lat", None, "ch"), check_vma=False
    )
```

```python
import functools
import math

import jax
import jax.numpy as jnp
from jax import lax
import numpy as np
from jax.experimental import pallas as pl
from jax.experimental.pallas import tpu as pltpu
from jax.sharding import PartitionSpec as P

D = 768
M = 64
STEPS = 4


EPS = 1e-05
SHRINK = 0.01
HIGH = lax.Precision.HIGHEST


def longitude_tables(width, modes):
    column = jnp.arange(width, dtype=jnp.int32)[:, None]
    order = jnp.arange(modes, dtype=jnp.int32)[None, :]
    angle = 2.0 * math.pi / width * (column * order % width).astype(jnp.float32)
    doubled = jnp.where(order == 0, 1.0, 2.0).astype(jnp.float32)
    return (jnp.cos(angle), jnp.sin(angle), jnp.cos(angle) * doubled, jnp.sin(angle) * doubled)


def latitude_tables(height):
    column = jnp.arange(height, dtype=jnp.int32)[:, None]
    order = jnp.arange(height, dtype=jnp.int32)[None, :]
    angle = 2.0 * math.pi / height * (column * order % height).astype(jnp.float32)
    return (jnp.cos(angle), jnp.sin(angle))


def layer_norm(values, gain, shift):
    mean = jnp.sum(values, -1, keepdims=True) / values.shape[-1]
    spread = jnp.sum(values * values, -1, keepdims=True) / values.shape[-1] - mean * mean
    return (values - mean) * lax.rsqrt(spread + EPS) * gain + shift


def soft_shrink(values):
    return jnp.where(
        values > SHRINK, values - SHRINK, jnp.where(values < -SHRINK, values + SHRINK, 0.0)
    )


def block_apply(left, matrix):
    return jnp.einsum("bkmnj,nji->bkmni", left, matrix, precision=HIGH)


def spectral_mlp(real_part, imag_part, filter_in, filter_in_bias, filter_out, filter_out_bias):
    shape = real_part.shape
    blocks = filter_in.shape[1]
    size = filter_in.shape[2]
    real_blocks = real_part.reshape(shape[:-1] + (blocks, size))
    imag_blocks = imag_part.reshape(shape[:-1] + (blocks, size))
    first_real = jax.nn.relu(
        block_apply(real_blocks, filter_in[0])
        - block_apply(imag_blocks, filter_in[1])
        + filter_in_bias[0]
    )
    first_imag = jax.nn.relu(
        block_apply(imag_blocks, filter_in[0])
        + block_apply(real_blocks, filter_in[1])
        + filter_in_bias[1]
    )
    second_real = (
        block_apply(first_real, filter_out[0])
        - block_apply(first_imag, filter_out[1])
        + filter_out_bias[0]
    )
    second_imag = (
        block_apply(first_imag, filter_out[0])
        + block_apply(first_real, filter_out[1])
        + filter_out_bias[1]
    )
    return (soft_shrink(second_real).reshape(shape), soft_shrink(second_imag).reshape(shape))


def local(
    state,
    norm_gains,
    channel_biases,
    filter_in,
    filter_in_bias,
    filter_out,
    filter_out_bias,
    up_weight,
    up_bias,
    down_weight,
):
    width = state.shape[2]
    height = state.shape[1] * lax.axis_size("lat")
    scale = 1.0 / math.sqrt(height * width)
    lon_cos, lon_sin, back_cos, back_sin = longitude_tables(width, M)
    lat_cos, lat_sin = latitude_tables(height)
    gains = norm_gains.astype(jnp.float32)
    shifts = channel_biases.astype(jnp.float32)
    full_up, full_gains, full_biases = (
        lax.all_gather(up_weight, "ch", axis=1, tiled=True),
        lax.all_gather(norm_gains, "ch", axis=1, tiled=True),
        lax.all_gather(channel_biases, "ch", axis=1, tiled=True),
    )
    full_down, full_up_bias = (
        lax.all_gather(down_weight, "ch", axis=0, tiled=True),
        lax.all_gather(up_bias, "ch", axis=0, tiled=True),
    )
    wide_gains = full_gains.astype(jnp.float32)
    wide_biases = full_biases.astype(jnp.float32)
    wide_up_bias = full_up_bias.astype(jnp.float32)
    values = state
    for step_index in range(STEPS):
        total, squares = lax.psum(
            (jnp.sum(values, -1, keepdims=True), jnp.sum(values * values, -1, keepdims=True)), "ch"
        )
        mean = total / D
        mean, spread = (mean, squares / D - mean * mean)
        normed = (values - mean) * lax.rsqrt(spread + EPS) * gains[0] + shifts[0]
        real_lon = jnp.einsum("bhwd,wm->bhmd", normed, lon_cos, precision=HIGH)
        imag_lon = -jnp.einsum("bhwd,wm->bhmd", normed, lon_sin, precision=HIGH)
        stacked = lax.all_to_all(
            jnp.stack((real_lon, imag_lon)), "lat", split_axis=3, concat_axis=2, tiled=True
        )
        spectral_real_lon = stacked[0]
        spectral_imag_lon = stacked[1]
        real_spec = (
            jnp.einsum("kh,bhmd->bkmd", lat_cos, spectral_real_lon, precision=HIGH)
            + jnp.einsum("kh,bhmd->bkmd", lat_sin, spectral_imag_lon, precision=HIGH)
        ) * scale
        imag_spec = (
            jnp.einsum("kh,bhmd->bkmd", lat_cos, spectral_imag_lon, precision=HIGH)
            - jnp.einsum("kh,bhmd->bkmd", lat_sin, spectral_real_lon, precision=HIGH)
        ) * scale
        out_real, out_imag = spectral_mlp(
            real_spec, imag_spec, filter_in, filter_in_bias, filter_out, filter_out_bias
        )
        real_rows = jnp.einsum("kh,bkmd->bhmd", lat_cos, out_real, precision=HIGH) - jnp.einsum(
            "kh,bkmd->bhmd", lat_sin, out_imag, precision=HIGH
        )
        imag_rows = jnp.einsum("kh,bkmd->bhmd", lat_cos, out_imag, precision=HIGH) + jnp.einsum(
            "kh,bkmd->bhmd", lat_sin, out_real, precision=HIGH
        )
        rows = lax.all_to_all(
            jnp.stack((real_rows, imag_rows)), "lat", split_axis=2, concat_axis=3, tiled=True
        )
        back = jnp.einsum("bhmd,wm->bhwd", rows[0], back_cos, precision=HIGH) - jnp.einsum(
            "bhmd,wm->bhwd", rows[1], back_sin, precision=HIGH
        )
        values = values + back * scale + normed
        owned = lax.all_to_all(values, "ch", split_axis=2, concat_axis=3, tiled=True)
        normed_two = layer_norm(owned, wide_gains[1], wide_biases[1]).astype(jnp.bfloat16)
        flat = normed_two.reshape(-1, normed_two.shape[-1])
        pre = jnp.dot(flat, full_up, preferred_element_type=jnp.float32) + wide_up_bias
        hidden = jax.nn.gelu(pre, approximate=False).astype(jnp.bfloat16)
        mixed = jnp.dot(hidden, full_down, preferred_element_type=jnp.float32) + wide_biases[2]
        values = values + lax.all_to_all(
            mixed.reshape(owned.shape), "ch", split_axis=3, concat_axis=2, tiled=True
        )
    return values


F32 = jnp.float32
BF16 = jnp.bfloat16
MESH = pl.DeviceIdType.MESH


def split_table(table):
    high = np.asarray(table, np.float32).astype(jnp.bfloat16)
    low = (table - high.astype(np.float64)).astype(np.float32).astype(jnp.bfloat16)
    return np.stack((high, low))


def fourier_tables(width, part, height, modes, owners):
    scale = 1.0 / math.sqrt(height * width)
    share = modes // owners
    rows = height // owners
    half = -(-width // 2)
    token = np.arange(width)
    place = token // half * part + token % half
    order = np.arange(modes).reshape(owners, share)
    angle = 2.0 * np.pi / width * (order[:, :, None] * token % width)
    forward = np.zeros((owners, 2, share, 2 * part))
    forward[:, 0, :, place] = np.moveaxis(np.cos(angle), -1, 0)
    forward[:, 1, :, place] = np.moveaxis(-np.sin(angle), -1, 0)
    doubled = np.where(order == 0, 1.0, 2.0)[:, None, :, None] * scale
    backward = (forward * doubled).reshape(2 * modes, 2 * part).T
    forward = forward.reshape(2 * modes, 2 * part)
    turns = np.arange(height)
    turn = 2.0 * np.pi / height * (turns[:, None] * turns[None, :] % height)
    cos, sin, eye = np.cos(turn), np.sin(turn), np.eye(share)
    mix = np.array([[cos, sin], [-sin, cos]])
    size = 2 * height * share
    lat = np.einsum("abkh,mn->akmhbn", mix, eye).reshape(size, size) * scale
    unmix = np.array([[cos, -sin], [sin, cos]])
    back = np.einsum("bahk,mn->hbmakn", unmix, eye)
    back = back.reshape((owners, rows) + back.shape[1:]).swapaxes(0, 1).reshape(size, size)
    return tuple(split_table(t) for t in (forward, lat, back, backward))


def dot(left, right):
    return jnp.dot(left, right, preferred_element_type=F32)


def halves(values):
    high = values.astype(BF16)
    return high, (values - high.astype(F32)).astype(BF16)


def dot3(left, right):
    return dot(left[0], right[0]) + dot(left[1], right[0]) + dot(left[0], right[1])


def gelu(values):
    return 0.5 * values * (1.0 + lax.erf(values * (1.0 / math.sqrt(2.0))))


def flip(index, bits):
    bit, moved = 1, index
    while bit <= bits:
        if bits & bit:
            moved = moved + bit - 2 * bit * lax.rem(lax.div(index, bit), 2)
        bit *= 2
    return moved


LANES = 128


def pack(values):
    rows = values.shape[-2] // 2
    rest = values[..., LANES:]
    folded = jnp.concatenate((rest[..., :rows, :], rest[..., rows:, :]), -1)
    return values[..., :LANES].astype(BF16), folded.astype(BF16)


def unfold(folded):
    values = folded.astype(F32)
    return jnp.concatenate((values[..., : LANES // 2], values[..., LANES // 2 :]), -2)


def store_packed(target, where, values):
    rows = values.shape[-2]
    full, folded = pack(values)
    target[where + (slice(0, rows),)] = full
    target[where + (slice(rows, rows + rows // 2),)] = folded


STAT, LON, ROW, TOK, MIX, SETUP = range(6)


def rollout(
    lats,
    chans,
    state_hbm,
    gains_hbm,
    shifts_hbm,
    fin_bias_hbm,
    fout_bias_hbm,
    up_bias_hbm,
    fin_hbm,
    fout_hbm,
    up_hbm,
    down_hbm,
    t_lon_hbm,
    t_lat_hbm,
    t_rows_hbm,
    t_back_hbm,
    out_hbm,
    state,
    gains,
    shifts,
    fin_bias,
    fout_bias,
    up_bias,
    x,
    stat_send,
    stat_recv,
    lon_send,
    lon_recv,
    row_send,
    row_recv,
    tok_send,
    tok_recv,
    mix_full,
    mix_send,
    mix_pair,
    mix_recv,
    bias_send,
    bias_recv,
    par_send,
    par_recv,
    par,
    fin_raw,
    fout_raw,
    fin,
    fout,
    fin_b,
    fout_b,
    up,
    down,
    up_recv,
    down_recv,
    t_lon,
    t_lat,
    t_rows,
    t_back,
    tokens,
    hidden,
    load_sem,
    send_sem,
    recv_sem,
):
    lat, ch = lax.axis_index("lat"), lax.axis_index("ch")
    core, chip = lax.rem(ch, 2), lax.div(ch, 2)
    chips = chans // 2
    rows, width, _, own = state.shape
    part = x.shape[2]
    near = -(-width // 2)
    wide = chans * own
    hid = up.shape[1]
    spread_modes = t_lon.shape[1]

    def chan(q):
        return 2 * lax.rem(chip + q // 2, chips) + (core if q % 2 == 0 else 1 - core)

    def half_of(q):
        return core if q % 2 == 0 else 1 - core

    up_rows = []
    for c in range(chans):
        up_rows.append((pl.ds(c * own, LANES), pl.ds(c * LANES, LANES)))
        rest = own - LANES
        up_rows.append((pl.ds(c * own + LANES, rest), pl.ds(chans * LANES + c * rest, rest)))

    lat_order = sorted(range(1, lats), key=lambda k: -4 * (2 * k // lats) - 2 * (k % 2) - k / lats)
    ch_order = tuple(range(2, chans)) + (1,)

    loads = [
        pltpu.make_async_copy(source, target, load_sem.at[n])
        for n, (source, target) in enumerate(
            (
                (state_hbm, state),
                (gains_hbm, gains),
                (shifts_hbm, shifts),
                (up_bias_hbm, up_bias),
                (fin_bias_hbm, fin_bias),
                (fout_bias_hbm, fout_bias),
                (fin_hbm, fin_raw),
                (fout_hbm, fout_raw),
                (t_lon_hbm, t_lon),
                (t_lat_hbm, t_lat),
                (t_rows_hbm, t_rows),
                (t_back_hbm, t_back),
                (down_hbm, down),
            )
            + tuple((up_hbm.at[source], up.at[target]) for source, target in up_rows)
        )
    ]
    for each in loads:
        each.start()
    stores = [
        pltpu.make_async_copy(state.at[r], out_hbm.at[r], load_sem.at[r]) for r in range(rows)
    ]

    barrier = pltpu.get_barrier_semaphore()
    for k in lat_order:
        pl.semaphore_signal(barrier, inc=1, device_id={"lat": flip(lat, k)}, device_id_type=MESH)
    for q in ch_order:
        pl.semaphore_signal(barrier, inc=1, device_id={"ch": chan(q)}, device_id_type=MESH)

    def copy(kind, r, k, source, target, device):
        return pltpu.make_async_remote_copy(
            src_ref=source,
            dst_ref=target,
            send_sem=send_sem.at[kind, r, k],
            recv_sem=recv_sem.at[kind, r, k],
            device_id=device,
            device_id_type=MESH,
        )

    def stat_copies(r):
        return [
            copy(STAT, r, q, stat_send.at[r], stat_recv.at[r, ch], {"ch": chan(q)})
            for q in ch_order
        ]

    def lon_copies(r):
        return [
            copy(LON, r, k, lon_send.at[r, flip(lat, k)], lon_recv.at[lat, r], {"lat": flip(lat, k)})
            for k in lat_order
        ]

    def row_copies(r):
        return [
            copy(ROW, r, k, row_send.at[r, flip(lat, k)], row_recv.at[r, lat], {"lat": flip(lat, k)})
            for k in lat_order
        ]

    def tok_copies(r):
        return [
            copy(TOK, r, q, tok_send.at[r, half_of(q)], tok_recv.at[r, ch], {"ch": chan(q)})
            for q in ch_order
        ]

    def mix_copy(r, q):
        if q == 1:
            return copy(MIX, r, q, mix_full.at[r, 1 - core], mix_pair.at[r], {"ch": chan(q)})
        n = q // 2 - 1
        source = mix_send.at[r, n, half_of(q)]
        return copy(MIX, r, q, source, mix_recv.at[r, n, core], {"ch": chan(q)})

    def mix_copies(r):
        return [mix_copy(r, q) for q in ch_order]

    def start(copies):
        for each in copies:
            each.start()

    def finish(copies):
        for each in copies:
            each.wait()

    x[...] = jnp.zeros_like(x)
    loads[0].wait()
    for r in range(rows):
        x[r, 0, 0:near] = state[r, 0:near, 0]
        x[r, 1, 0 : width - near] = state[r, near:width, 0]
    ones = jnp.ones((8, own), BF16)
    which = lax.broadcasted_iota(jnp.int32, (8, 2 * part), 0)

    def row_sums(values):
        dims = (((1,), (1,)), ((), ()))
        high, low = halves(values)
        return lax.dot_general(
            ones, high, dims, preferred_element_type=F32
        ) + lax.dot_general(ones, low, dims, preferred_element_type=F32)

    def own_stats(r):
        values = x[r].reshape(2 * part, own)
        sums = jnp.where(which == 0, row_sums(values), row_sums(values * values))
        stat_send[r] = sums
        stat_recv[r, pl.ds(ch, 1)] = sums[None]

    def take_stats(r):
        with jax.named_scope("wait_stat"):
            finish(stat_copies(r))
        total = stat_recv[r, 0]
        for c in range(1, chans):
            total = total + stat_recv[r, c]
        mean = total[0:1] / wide
        scaled = lax.rsqrt(total[1:2] / wide - mean * mean + EPS)
        both = jnp.transpose(jnp.where(which == 0, mean, scaled))
        return both[:, 0:1], both[:, 1:2]

    for r in range(rows):
        own_stats(r)
    pl.semaphore_wait(barrier, lats + chans - 2)
    for r in range(rows):
        start(stat_copies(r))
    for each in loads[1:4]:
        each.wait()
    gain = gains[...].astype(F32)
    shift = shifts[...].astype(F32)
    par_send[...] = jnp.concatenate((gain[1:2], shift[1:2], jnp.zeros((6, own), F32)), 0)
    par_recv[pl.ds(ch, 1)] = par_send[...][None]
    bias_send[...] = jnp.broadcast_to(up_bias[...].astype(F32)[None], bias_send.shape)
    partner = {"ch": chan(1)}
    setup = [
        copy(SETUP, 0, 0, down_hbm, down_recv, partner),
        copy(SETUP, 0, 1, bias_send, bias_recv, partner),
    ]
    for n, (source, target) in enumerate(up_rows):
        setup.append(
            copy(SETUP, 1 + n // chans, n % chans, up_hbm.at[source], up_recv.at[target], partner)
        )
    for n, q in enumerate(ch_order):
        setup.append(copy(SETUP, 0, 2 + n, par_send, par_recv.at[ch], {"ch": chan(q)}))
    start(setup)
    for each in loads[4:8]:
        each.wait()
    blocks, size = fin_raw.shape[1], fin_raw.shape[2]
    line = lax.broadcasted_iota(jnp.int32, (size, own), 0)
    lane = lax.broadcasted_iota(jnp.int32, (size, own), 1)
    for raw, target, bias, bias_target in (
        (fin_raw, fin, fin_bias, fin_b),
        (fout_raw, fout, fout_bias, fout_b),
    ):
        placed = 0.0
        for n in range(blocks):
            shifted = jnp.where(lane == line + n * size, 1.0, 0.0)
            select = shifted.astype(BF16)
            for p in range(2):
                high, low = halves(raw[p, n])
                target[p, 0, n * size : (n + 1) * size] = dot(high, select).astype(BF16)
                target[p, 1, n * size : (n + 1) * size] = dot(low, select).astype(BF16)
            placed = placed + jnp.dot(
                bias[:, n, :], shifted, precision=HIGH, preferred_element_type=F32
            )
        bias_target[...] = placed
    for each in loads[8:12]:
        each.wait()

    def complex_apply(pair, weights, bias):
        split = pair.shape[0] // 2
        pair = halves(pair)
        one = dot3(pair, (weights[0, 0], weights[0, 1]))
        two = dot3(pair, (weights[1, 0], weights[1, 1]))
        return (
            one[:split] - two[split:] + bias[0:1, :],
            one[split:] + two[:split] + bias[1:2, :],
        )

    def spectrum(messages, count):
        full = messages[..., :count, :]
        rest = unfold(messages[..., count:, :]).astype(BF16)
        return jnp.concatenate((full, rest), -1).reshape(-1, own)

    share = spread_modes // lats

    def forward(r):
        with jax.named_scope("forward"):
            mean, scaled = take_stats(r)
            now = x[r].reshape(2 * part, own)
            normed = (now - mean) * scaled * gain[0:1] + shift[0:1]
            x[r] = (now + normed).reshape(2, part, own)
            spectra = dot3((t_lon[0], t_lon[1]), halves(normed))
            store_packed(lon_send, (r, slice(None)), spectra.reshape(lats, share, own))
            start(lon_copies(r))
            lon_recv[pl.ds(lat, 1), r] = lon_send[r, pl.ds(lat, 1)]

    def spectral():
        data = spectrum(lon_recv[...], share)
        spec = dot(t_lat[0], data) + dot(t_lat[1], data)
        real, imag = complex_apply(spec, fin, fin_b)
        pair = jnp.concatenate((jnp.maximum(real, 0.0), jnp.maximum(imag, 0.0)), 0)
        real, imag = complex_apply(pair, fout, fout_b)
        return halves(jnp.concatenate((soft_shrink(real), soft_shrink(imag)), 0))

    def unmix(r, pair):
        cut = slice(r * spread_modes, (r + 1) * spread_modes)
        back = dot3((t_rows[0, cut], t_rows[1, cut]), pair)
        store_packed(row_send, (r, slice(None)), back.reshape(lats, share, own))
        start(row_copies(r))
        row_recv[r, pl.ds(lat, 1)] = row_send[r, pl.ds(lat, 1)]

    def backward(r):
        data = spectrum(row_recv[r], share)
        back = dot(t_back[0], data) + dot(t_back[1], data)
        now = x[r] + back.reshape(2, part, own)
        x[r] = now
        store_packed(tok_send, (r, slice(None)), now)
        start(tok_copies(r))
        tok_recv[r, pl.ds(ch, 1)] = tok_send[r, pl.ds(core, 1)]

    def token_piece(r, n):
        if n < chans:
            return tok_recv[r, n, 0:part].astype(F32)
        c = 2 * (n - chans)
        one = tok_recv[r, c, part : part + part // 2].astype(F32)
        two = tok_recv[r, c + 1, part : part + part // 2].astype(F32)
        rest = LANES // 2
        upper = jnp.concatenate((one[:, :rest], two[:, :rest]), -1)
        lower = jnp.concatenate((one[:, rest:], two[:, rest:]), -1)
        return jnp.concatenate((upper, lower), 0)

    def project_up(r):
        total, squares = 0.0, 0.0
        for n in range(wide // LANES):
            piece = token_piece(r, n)
            total = total + piece
            squares = squares + piece * piece
        mean = jnp.sum(total, -1, keepdims=True) / wide
        spread = jnp.sum(squares, -1, keepdims=True) / wide - mean * mean
        scaled = lax.rsqrt(spread + EPS)
        for n in range(wide // LANES):
            cut = slice(n * LANES, (n + 1) * LANES)
            normed = (token_piece(r, n) - mean) * scaled * par[0:1, cut] + par[1:2, cut]
            tokens[0:part, cut], tokens[part : 2 * part, cut] = halves(normed)
        for s, (weight, bias) in enumerate(((up, bias_send), (up_recv, bias_recv))):
            for lo in range(0, hid, 256):
                cut = slice(lo, lo + 256)
                both = dot(tokens[...], weight[:, cut])
                pre = both[:part] + both[part:] + bias[0:1, cut]
                hidden[s, :, cut] = gelu(pre).astype(BF16)

    def project_down(r):
        for j in tuple(range(1, chips)) + (0,):
            first = pl.multiple_of(2 * own * lax.rem(chip + j, chips), LANES)
            cut = pl.ds(first, 2 * own)
            mixed = dot(hidden[0], down[:, cut]) + dot(hidden[1], down_recv[:, cut])
            for n in range(2):
                piece = mixed[:, n * own : (n + 1) * own]
                if j:
                    store_packed(mix_send, (r, j - 1, n), piece)
                else:
                    mix_full[r, n] = piece
            for q in (2 * j, 2 * j + 1):
                if q:
                    mix_copy(r, q).start()

    def residual(r):
        for h, piece in ((core, mix_full[r, pl.ds(core, 1)]), (1 - core, mix_pair[r][None])):
            for n in range(chips - 1):
                message = mix_recv[r, n, pl.ds(h, 1)]
                rest = unfold(message[:, part:])
                piece = piece + jnp.concatenate((message[:, :part].astype(F32), rest), -1)
            x[r, pl.ds(h, 1)] = x[r, pl.ds(h, 1)] + piece + shift[2:3]

    @pl.loop(0, STEPS)
    def _(index):
        for r in range(rows):
            forward(r)
        with jax.named_scope("wait_lon"):
            for r in range(rows):
                finish(lon_copies(r))
        with jax.named_scope("spectral"):
            pair = spectral()
        with jax.named_scope("unmix"):
            for r in range(rows):
                unmix(r, pair)
        for r in range(rows):
            with jax.named_scope("wait_row"):
                finish(row_copies(r))
            with jax.named_scope("backward"):
                backward(r)

        @pl.when(index == 0)
        def _():
            for each in loads[12:]:
                each.wait()
            finish(setup)
            pieces = [par_recv[c, 0:2, :LANES] for c in range(chans)]
            pieces += [par_recv[c, 0:2, LANES:] for c in range(chans)]
            par[...] = jnp.concatenate(pieces, -1)

        for r in range(rows):
            with jax.named_scope("wait_tok"):
                finish(tok_copies(r))
            with jax.named_scope("up"):
                project_up(r)
            with jax.named_scope("down"):
                project_down(r)
        for r in range(rows):
            with jax.named_scope("wait_mix"):
                finish(mix_copies(r))
            with jax.named_scope("residual"):
                residual(r)

            @pl.when(index == STEPS - 1)
            def _():
                state[r, 0:near, 0] = x[r, 0, 0:near]
                state[r, near:width, 0] = x[r, 1, 0 : width - near]
                stores[r].start()

            @pl.when(index < STEPS - 1)
            def _():
                own_stats(r)
                start(stat_copies(r))

    for each in stores:
        each.wait()


def fused(
    lats,
    chans,
    state,
    norm_gains,
    channel_biases,
    filter_in,
    filter_in_bias,
    filter_out,
    filter_out_bias,
    up_weight,
    up_bias,
    down_weight,
):
    _, rows, width, own = state.shape
    part = -(--(-width // 2) // 16) * 16
    share = 2 * M // lats
    hid = up_weight.shape[1]
    tables = tuple(
        jnp.asarray(t) for t in fourier_tables(width, part, rows * lats, M, lats)
    )
    args = (
        state.transpose(1, 2, 0, 3),
        norm_gains,
        channel_biases,
        filter_in_bias,
        filter_out_bias,
        up_bias,
        filter_in,
        filter_out,
        up_weight,
        down_weight,
    ) + tables
    hbm = pl.BlockSpec(memory_space=pltpu.HBM)
    packed = share + share // 2
    spectrum = (rows, lats, packed, LANES)
    folded = part + part // 2
    peers = max(lats, chans)
    result = pl.pallas_call(
        functools.partial(rollout, lats, chans),
        out_shape=jax.ShapeDtypeStruct((rows, width, 1, own), F32),
        in_specs=[hbm] * 14,
        out_specs=hbm,
        scratch_shapes=[
            pltpu.VMEM((rows, width, 1, own), F32),
            pltpu.VMEM(norm_gains.shape, BF16),
            pltpu.VMEM(channel_biases.shape, BF16),
            pltpu.VMEM(filter_in_bias.shape, F32),
            pltpu.VMEM(filter_out_bias.shape, F32),
            pltpu.VMEM(up_bias.shape, BF16),
            pltpu.VMEM((rows, 2, part, own), F32),
            pltpu.VMEM((rows, 8, 2 * part), F32),
            pltpu.VMEM((rows, chans, 8, 2 * part), F32),
            pltpu.VMEM(spectrum, BF16),
            pltpu.VMEM((lats, rows, packed, LANES), BF16),
            pltpu.VMEM(spectrum, BF16),
            pltpu.VMEM(spectrum, BF16),
            pltpu.VMEM((rows, 2, folded, LANES), BF16),
            pltpu.VMEM((rows, chans, folded, LANES), BF16),
            pltpu.VMEM((rows, 2, part, own), F32),
            pltpu.VMEM((rows, chans // 2 - 1, 2, folded, LANES), BF16),
            pltpu.VMEM((rows, part, own), F32),
            pltpu.VMEM((rows, chans // 2 - 1, 2, folded, LANES), BF16),
            pltpu.VMEM((8, hid), F32),
            pltpu.VMEM((8, hid), F32),
            pltpu.VMEM((8, own), F32),
            pltpu.VMEM((chans, 8, own), F32),
            pltpu.VMEM((2, chans * own), F32),
            pltpu.VMEM(filter_in.shape, F32),
            pltpu.VMEM(filter_out.shape, F32),
            pltpu.VMEM((2, 2, own, own), BF16),
            pltpu.VMEM((2, 2, own, own), BF16),
            pltpu.VMEM((2, own), F32),
            pltpu.VMEM((2, own), F32),
            pltpu.VMEM(up_weight.shape, BF16),
            pltpu.VMEM(down_weight.shape, BF16),
            pltpu.VMEM(up_weight.shape, BF16),
            pltpu.VMEM(down_weight.shape, BF16),
        ]
        + [pltpu.VMEM(t.shape, BF16) for t in tables]
        + [
            pltpu.VMEM((2 * part, chans * own), BF16),
            pltpu.VMEM((2, part, hid), BF16),
            pltpu.SemaphoreType.DMA((13 + 2 * chans,)),
            pltpu.SemaphoreType.DMA((6, max(rows, 3), peers)),
            pltpu.SemaphoreType.DMA((6, max(rows, 3), peers)),
        ],
        compiler_params=pltpu.CompilerParams(
            collective_id=0, has_side_effects=True, vmem_limit_bytes=60 * 1024 * 1024
        ),
    )(*args)
    return result.transpose(2, 0, 1, 3)


def dispatch(sizes, *args):
    lats, chans = sizes["lat"], sizes["ch"]
    own = args[0].shape[3]
    folds = own // LANES == 1 and 2 * (own % LANES) == LANES
    if folds and 2 * M // lats % 16 == 0 and chans > 2 and chans % 2 == 0:
        return fused(lats, chans, *args)
    return local(*args)


def solution(mesh):
    placed = (
        P(None, "lat", None, "ch"),
        P(None, "ch"),
        P(None, "ch"),
        P(None, "ch", None, None),
        P(None, "ch", None),
        P(None, "ch", None, None),
        P(None, "ch", None),
        P(None, "ch"),
        P("ch"),
        P("ch", None),
    )
    return jax.shard_map(
        functools.partial(dispatch, dict(mesh.shape)), mesh=mesh, in_specs=placed, out_specs=P(None, "lat", None, "ch"), check_vma=False
    )
```

```python
import functools
import math

import jax
import jax.numpy as jnp
from jax import lax
import numpy as np
from jax.experimental import pallas as pl
from jax.experimental.pallas import tpu as pltpu
from jax.sharding import PartitionSpec as P

D = 768
M = 64
STEPS = 4


EPS = 1e-05
SHRINK = 0.01
HIGH = lax.Precision.HIGHEST


def longitude_tables(width, modes):
    column = jnp.arange(width, dtype=jnp.int32)[:, None]
    order = jnp.arange(modes, dtype=jnp.int32)[None, :]
    angle = 2.0 * math.pi / width * (column * order % width).astype(jnp.float32)
    doubled = jnp.where(order == 0, 1.0, 2.0).astype(jnp.float32)
    return (jnp.cos(angle), jnp.sin(angle), jnp.cos(angle) * doubled, jnp.sin(angle) * doubled)


def latitude_tables(height):
    column = jnp.arange(height, dtype=jnp.int32)[:, None]
    order = jnp.arange(height, dtype=jnp.int32)[None, :]
    angle = 2.0 * math.pi / height * (column * order % height).astype(jnp.float32)
    return (jnp.cos(angle), jnp.sin(angle))


def layer_norm(values, gain, shift):
    mean = jnp.sum(values, -1, keepdims=True) / values.shape[-1]
    spread = jnp.sum(values * values, -1, keepdims=True) / values.shape[-1] - mean * mean
    return (values - mean) * lax.rsqrt(spread + EPS) * gain + shift


def soft_shrink(values):
    return jnp.where(
        values > SHRINK, values - SHRINK, jnp.where(values < -SHRINK, values + SHRINK, 0.0)
    )


def block_apply(left, matrix):
    return jnp.einsum("bkmnj,nji->bkmni", left, matrix, precision=HIGH)


def spectral_mlp(real_part, imag_part, filter_in, filter_in_bias, filter_out, filter_out_bias):
    shape = real_part.shape
    blocks = filter_in.shape[1]
    size = filter_in.shape[2]
    real_blocks = real_part.reshape(shape[:-1] + (blocks, size))
    imag_blocks = imag_part.reshape(shape[:-1] + (blocks, size))
    first_real = jax.nn.relu(
        block_apply(real_blocks, filter_in[0])
        - block_apply(imag_blocks, filter_in[1])
        + filter_in_bias[0]
    )
    first_imag = jax.nn.relu(
        block_apply(imag_blocks, filter_in[0])
        + block_apply(real_blocks, filter_in[1])
        + filter_in_bias[1]
    )
    second_real = (
        block_apply(first_real, filter_out[0])
        - block_apply(first_imag, filter_out[1])
        + filter_out_bias[0]
    )
    second_imag = (
        block_apply(first_imag, filter_out[0])
        + block_apply(first_real, filter_out[1])
        + filter_out_bias[1]
    )
    return (soft_shrink(second_real).reshape(shape), soft_shrink(second_imag).reshape(shape))


def local(
    state,
    norm_gains,
    channel_biases,
    filter_in,
    filter_in_bias,
    filter_out,
    filter_out_bias,
    up_weight,
    up_bias,
    down_weight,
):
    width = state.shape[2]
    height = state.shape[1] * lax.axis_size("lat")
    scale = 1.0 / math.sqrt(height * width)
    lon_cos, lon_sin, back_cos, back_sin = longitude_tables(width, M)
    lat_cos, lat_sin = latitude_tables(height)
    gains = norm_gains.astype(jnp.float32)
    shifts = channel_biases.astype(jnp.float32)
    full_up, full_gains, full_biases = (
        lax.all_gather(up_weight, "ch", axis=1, tiled=True),
        lax.all_gather(norm_gains, "ch", axis=1, tiled=True),
        lax.all_gather(channel_biases, "ch", axis=1, tiled=True),
    )
    full_down, full_up_bias = (
        lax.all_gather(down_weight, "ch", axis=0, tiled=True),
        lax.all_gather(up_bias, "ch", axis=0, tiled=True),
    )
    wide_gains = full_gains.astype(jnp.float32)
    wide_biases = full_biases.astype(jnp.float32)
    wide_up_bias = full_up_bias.astype(jnp.float32)
    values = state
    for step_index in range(STEPS):
        total, squares = lax.psum(
            (jnp.sum(values, -1, keepdims=True), jnp.sum(values * values, -1, keepdims=True)), "ch"
        )
        mean = total / D
        mean, spread = (mean, squares / D - mean * mean)
        normed = (values - mean) * lax.rsqrt(spread + EPS) * gains[0] + shifts[0]
        real_lon = jnp.einsum("bhwd,wm->bhmd", normed, lon_cos, precision=HIGH)
        imag_lon = -jnp.einsum("bhwd,wm->bhmd", normed, lon_sin, precision=HIGH)
        stacked = lax.all_to_all(
            jnp.stack((real_lon, imag_lon)), "lat", split_axis=3, concat_axis=2, tiled=True
        )
        spectral_real_lon = stacked[0]
        spectral_imag_lon = stacked[1]
        real_spec = (
            jnp.einsum("kh,bhmd->bkmd", lat_cos, spectral_real_lon, precision=HIGH)
            + jnp.einsum("kh,bhmd->bkmd", lat_sin, spectral_imag_lon, precision=HIGH)
        ) * scale
        imag_spec = (
            jnp.einsum("kh,bhmd->bkmd", lat_cos, spectral_imag_lon, precision=HIGH)
            - jnp.einsum("kh,bhmd->bkmd", lat_sin, spectral_real_lon, precision=HIGH)
        ) * scale
        out_real, out_imag = spectral_mlp(
            real_spec, imag_spec, filter_in, filter_in_bias, filter_out, filter_out_bias
        )
        real_rows = jnp.einsum("kh,bkmd->bhmd", lat_cos, out_real, precision=HIGH) - jnp.einsum(
            "kh,bkmd->bhmd", lat_sin, out_imag, precision=HIGH
        )
        imag_rows = jnp.einsum("kh,bkmd->bhmd", lat_cos, out_imag, precision=HIGH) + jnp.einsum(
            "kh,bkmd->bhmd", lat_sin, out_real, precision=HIGH
        )
        rows = lax.all_to_all(
            jnp.stack((real_rows, imag_rows)), "lat", split_axis=2, concat_axis=3, tiled=True
        )
        back = jnp.einsum("bhmd,wm->bhwd", rows[0], back_cos, precision=HIGH) - jnp.einsum(
            "bhmd,wm->bhwd", rows[1], back_sin, precision=HIGH
        )
        values = values + back * scale + normed
        owned = lax.all_to_all(values, "ch", split_axis=2, concat_axis=3, tiled=True)
        normed_two = layer_norm(owned, wide_gains[1], wide_biases[1]).astype(jnp.bfloat16)
        flat = normed_two.reshape(-1, normed_two.shape[-1])
        pre = jnp.dot(flat, full_up, preferred_element_type=jnp.float32) + wide_up_bias
        hidden = jax.nn.gelu(pre, approximate=False).astype(jnp.bfloat16)
        mixed = jnp.dot(hidden, full_down, preferred_element_type=jnp.float32) + wide_biases[2]
        values = values + lax.all_to_all(
            mixed.reshape(owned.shape), "ch", split_axis=3, concat_axis=2, tiled=True
        )
    return values


F32 = jnp.float32
BF16 = jnp.bfloat16
MESH = pl.DeviceIdType.MESH


def split_table(table):
    high = np.asarray(table, np.float32).astype(jnp.bfloat16)
    low = (table - high.astype(np.float64)).astype(np.float32).astype(jnp.bfloat16)
    return np.stack((high, low))


def fourier_tables(width, part, height, modes, owners):
    scale = 1.0 / math.sqrt(height * width)
    share = modes // owners
    rows = height // owners
    half = -(-width // 2)
    token = np.arange(width)
    place = token // half * part + token % half
    order = np.arange(modes).reshape(owners, share)
    angle = 2.0 * np.pi / width * (order[:, :, None] * token % width)
    forward = np.zeros((owners, 2, share, 2 * part))
    forward[:, 0, :, place] = np.moveaxis(np.cos(angle), -1, 0)
    forward[:, 1, :, place] = np.moveaxis(-np.sin(angle), -1, 0)
    doubled = np.where(order == 0, 1.0, 2.0)[:, None, :, None] * scale
    backward = (forward * doubled).reshape(2 * modes, 2 * part).T
    forward = forward.reshape(2 * modes, 2 * part)
    turns = np.arange(height)
    turn = 2.0 * np.pi / height * (turns[:, None] * turns[None, :] % height)
    cos, sin, eye = np.cos(turn), np.sin(turn), np.eye(share)
    mix = np.array([[cos, sin], [-sin, cos]])
    size = 2 * height * share
    lat = np.einsum("abkh,mn->akmhbn", mix, eye).reshape(size, size) * scale
    unmix = np.array([[cos, -sin], [sin, cos]])
    back = np.einsum("bahk,mn->hbmakn", unmix, eye)
    back = back.reshape((owners, rows) + back.shape[1:]).swapaxes(0, 1).reshape(size, size)
    return tuple(split_table(t) for t in (forward, lat, back, backward))


def dot(left, right):
    return jnp.dot(left, right, preferred_element_type=F32)


def halves(values):
    high = values.astype(BF16)
    return high, (values - high.astype(F32)).astype(BF16)


def dot3(left, right):
    return dot(left[0], right[0]) + dot(left[1], right[0]) + dot(left[0], right[1])


def gelu(values):
    return 0.5 * values * (1.0 + lax.erf(values * (1.0 / math.sqrt(2.0))))


def flip(index, bits):
    bit, moved = 1, index
    while bit <= bits:
        if bits & bit:
            moved = moved + bit - 2 * bit * lax.rem(lax.div(index, bit), 2)
        bit *= 2
    return moved


LANES = 128


def pack(values):
    rows = values.shape[-2] // 2
    rest = values[..., LANES:]
    folded = jnp.concatenate((rest[..., :rows, :], rest[..., rows:, :]), -1)
    return values[..., :LANES].astype(BF16), folded.astype(BF16)


def unfold(folded):
    values = folded.astype(F32)
    return jnp.concatenate((values[..., : LANES // 2], values[..., LANES // 2 :]), -2)


def store_packed(target, where, values):
    rows = values.shape[-2]
    full, folded = pack(values)
    target[where + (slice(0, rows),)] = full
    target[where + (slice(rows, rows + rows // 2),)] = folded


STAT, LON, ROW, TOK, MIX, SETUP = range(6)


def rollout(
    lats,
    chans,
    state_hbm,
    gains_hbm,
    shifts_hbm,
    fin_bias_hbm,
    fout_bias_hbm,
    up_bias_hbm,
    fin_hbm,
    fout_hbm,
    up_hbm,
    down_hbm,
    t_lon_hbm,
    t_lat_hbm,
    t_rows_hbm,
    t_back_hbm,
    out_hbm,
    state,
    gains,
    shifts,
    fin_bias,
    fout_bias,
    up_bias,
    x,
    stat_send,
    stat_recv,
    lon_send,
    lon_recv,
    row_send,
    row_recv,
    tok_send,
    tok_recv,
    mix_full,
    mix_send,
    mix_pair,
    mix_recv,
    bias_send,
    bias_recv,
    par_send,
    par_recv,
    par,
    fin_raw,
    fout_raw,
    fin,
    fout,
    fin_b,
    fout_b,
    up,
    down,
    up_recv,
    down_recv,
    t_lon,
    t_lat,
    t_rows,
    t_back,
    tokens,
    hidden,
    load_sem,
    send_sem,
    recv_sem,
):
    lat, ch = lax.axis_index("lat"), lax.axis_index("ch")
    core, chip = lax.rem(ch, 2), lax.div(ch, 2)
    chips = chans // 2
    rows, width, _, own = state.shape
    part = x.shape[2]
    near = -(-width // 2)
    wide = chans * own
    hid = up.shape[1]
    spread_modes = t_lon.shape[1]

    def chan(q):
        return 2 * lax.rem(chip + q // 2, chips) + (core if q % 2 == 0 else 1 - core)

    def half_of(q):
        return core if q % 2 == 0 else 1 - core

    up_rows = []
    for c in range(chans):
        up_rows.append((pl.ds(c * own, LANES), pl.ds(c * LANES, LANES)))
        rest = own - LANES
        up_rows.append((pl.ds(c * own + LANES, rest), pl.ds(chans * LANES + c * rest, rest)))

    lat_order = sorted(range(1, lats), key=lambda k: -4 * (2 * k // lats) - 2 * (k % 2) - k / lats)
    ch_order = tuple(range(2, chans)) + (1,)

    loads = [
        pltpu.make_async_copy(source, target, load_sem.at[n])
        for n, (source, target) in enumerate(
            (
                (state_hbm, state),
                (gains_hbm, gains),
                (shifts_hbm, shifts),
                (up_bias_hbm, up_bias),
                (fin_bias_hbm, fin_bias),
                (fout_bias_hbm, fout_bias),
                (fin_hbm, fin_raw),
                (fout_hbm, fout_raw),
                (t_lon_hbm, t_lon),
                (t_lat_hbm, t_lat),
                (t_rows_hbm, t_rows),
                (t_back_hbm, t_back),
                (down_hbm, down),
            )
            + tuple((up_hbm.at[source], up.at[target]) for source, target in up_rows)
        )
    ]
    for each in loads:
        each.start()
    stores = [
        pltpu.make_async_copy(state.at[r], out_hbm.at[r], load_sem.at[r]) for r in range(rows)
    ]

    barrier = pltpu.get_barrier_semaphore()
    for k in lat_order:
        pl.semaphore_signal(barrier, inc=1, device_id={"lat": flip(lat, k)}, device_id_type=MESH)
    for q in ch_order:
        pl.semaphore_signal(barrier, inc=1, device_id={"ch": chan(q)}, device_id_type=MESH)

    def copy(kind, r, k, source, target, device):
        return pltpu.make_async_remote_copy(
            src_ref=source,
            dst_ref=target,
            send_sem=send_sem.at[kind, r, k],
            recv_sem=recv_sem.at[kind, r, k],
            device_id=device,
            device_id_type=MESH,
        )

    def stat_copies(r):
        return [
            copy(STAT, r, q, stat_send.at[r], stat_recv.at[r, ch], {"ch": chan(q)})
            for q in ch_order
        ]

    def lon_copies(r):
        return [
            copy(LON, r, k, lon_send.at[r, flip(lat, k)], lon_recv.at[lat, r], {"lat": flip(lat, k)})
            for k in lat_order
        ]

    def row_copies(r):
        return [
            copy(ROW, r, k, row_send.at[r, flip(lat, k)], row_recv.at[r, lat], {"lat": flip(lat, k)})
            for k in lat_order
        ]

    def tok_copies(r):
        return [
            copy(TOK, r, q, tok_send.at[r, half_of(q)], tok_recv.at[r, ch], {"ch": chan(q)})
            for q in ch_order
        ]

    def mix_copy(r, q):
        if q == 1:
            return copy(MIX, r, q, mix_full.at[r, 1 - core], mix_pair.at[r], {"ch": chan(q)})
        n = q // 2 - 1
        source = mix_send.at[r, n, half_of(q)]
        return copy(MIX, r, q, source, mix_recv.at[r, n, core], {"ch": chan(q)})

    def mix_copies(r):
        return [mix_copy(r, q) for q in ch_order]

    def start(copies):
        for each in copies:
            each.start()

    def finish(copies):
        for each in copies:
            each.wait()

    x[...] = jnp.zeros_like(x)
    loads[0].wait()
    for r in range(rows):
        x[r, 0, 0:near] = state[r, 0:near, 0]
        x[r, 1, 0 : width - near] = state[r, near:width, 0]
    ones = jnp.ones((8, own), BF16)
    which = lax.broadcasted_iota(jnp.int32, (8, 2 * part), 0)

    def row_sums(values):
        dims = (((1,), (1,)), ((), ()))
        high, low = halves(values)
        return lax.dot_general(
            ones, high, dims, preferred_element_type=F32
        ) + lax.dot_general(ones, low, dims, preferred_element_type=F32)

    def own_stats(r):
        values = x[r].reshape(2 * part, own)
        sums = jnp.where(which == 0, row_sums(values), row_sums(values * values))
        stat_send[r] = sums[0:2]
        stat_recv[r, pl.ds(ch, 1)] = sums[None, 0:2]

    def take_stats(r):
        with jax.named_scope("wait_stat"):
            finish(stat_copies(r))
        total = stat_recv[r, 0]
        for c in range(1, chans):
            total = total + stat_recv[r, c]
        mean = total[0:1] / wide
        scaled = lax.rsqrt(total[1:2] / wide - mean * mean + EPS)
        both = jnp.transpose(jnp.where(which == 0, mean, scaled))
        return both[:, 0:1], both[:, 1:2]

    for r in range(rows):
        own_stats(r)
    pl.semaphore_wait(barrier, lats + chans - 2)
    for r in range(rows):
        start(stat_copies(r))
    for each in loads[1:4]:
        each.wait()
    gain = gains[...].astype(F32)
    shift = shifts[...].astype(F32)
    par_send[...] = jnp.concatenate((gain[1:2], shift[1:2], jnp.zeros((6, own), F32)), 0)
    par_recv[pl.ds(ch, 1)] = par_send[...][None]
    bias_send[...] = jnp.broadcast_to(up_bias[...].astype(F32)[None], bias_send.shape)
    partner = {"ch": chan(1)}
    setup = [
        copy(SETUP, 0, 0, down_hbm, down_recv, partner),
        copy(SETUP, 0, 1, bias_send, bias_recv, partner),
    ]
    for n, (source, target) in enumerate(up_rows):
        setup.append(
            copy(SETUP, 1 + n // chans, n % chans, up_hbm.at[source], up_recv.at[target], partner)
        )
    for n, q in enumerate(ch_order):
        setup.append(copy(SETUP, 0, 2 + n, par_send, par_recv.at[ch], {"ch": chan(q)}))
    start(setup)
    for each in loads[4:8]:
        each.wait()
    blocks, size = fin_raw.shape[1], fin_raw.shape[2]
    line = lax.broadcasted_iota(jnp.int32, (size, own), 0)
    lane = lax.broadcasted_iota(jnp.int32, (size, own), 1)
    for raw, target, bias, bias_target in (
        (fin_raw, fin, fin_bias, fin_b),
        (fout_raw, fout, fout_bias, fout_b),
    ):
        placed = 0.0
        for n in range(blocks):
            shifted = jnp.where(lane == line + n * size, 1.0, 0.0)
            select = shifted.astype(BF16)
            for p in range(2):
                high, low = halves(raw[p, n])
                target[p, 0, n * size : (n + 1) * size] = dot(high, select).astype(BF16)
                target[p, 1, n * size : (n + 1) * size] = dot(low, select).astype(BF16)
            placed = placed + jnp.dot(
                bias[:, n, :], shifted, precision=HIGH, preferred_element_type=F32
            )
        bias_target[...] = placed
    for each in loads[8:12]:
        each.wait()

    def complex_apply(pair, weights, bias):
        split = pair.shape[0] // 2
        pair = halves(pair)
        one = dot3(pair, (weights[0, 0], weights[0, 1]))
        two = dot3(pair, (weights[1, 0], weights[1, 1]))
        return (
            one[:split] - two[split:] + bias[0:1, :],
            one[split:] + two[:split] + bias[1:2, :],
        )

    def spectrum(messages, count):
        full = messages[..., :count, :]
        rest = unfold(messages[..., count:, :]).astype(BF16)
        return jnp.concatenate((full, rest), -1).reshape(-1, own)

    share = spread_modes // lats

    def forward(r):
        with jax.named_scope("forward"):
            mean, scaled = take_stats(r)
            now = x[r].reshape(2 * part, own)
            normed = (now - mean) * scaled * gain[0:1] + shift[0:1]
            x[r] = (now + normed).reshape(2, part, own)
            spectra = dot3((t_lon[0], t_lon[1]), halves(normed))
            store_packed(lon_send, (r, slice(None)), spectra.reshape(lats, share, own))
            start(lon_copies(r))
            lon_recv[pl.ds(lat, 1), r] = lon_send[r, pl.ds(lat, 1)]

    def spectral():
        data = spectrum(lon_recv[...], share)
        size = t_lat.shape[1] // 4
        spec = []
        for n in range(4):
            cut = slice(n * size, (n + 1) * size)
            spec.append(dot(t_lat[0, cut], data) + dot(t_lat[1, cut], data))
        spec = jnp.concatenate(spec, 0)
        real, imag = complex_apply(spec, fin, fin_b)
        pair = jnp.concatenate((jnp.maximum(real, 0.0), jnp.maximum(imag, 0.0)), 0)
        real, imag = complex_apply(pair, fout, fout_b)
        return halves(jnp.concatenate((soft_shrink(real), soft_shrink(imag)), 0))

    def unmix(r, pair):
        count = spread_modes // 2
        for n in range(2):
            first = r * spread_modes + n * count
            cut = slice(first, first + count)
            back = dot3((t_rows[0, cut], t_rows[1, cut]), pair)
            where = (r, slice(n * lats // 2, (n + 1) * lats // 2))
            store_packed(row_send, where, back.reshape(lats // 2, share, own))
        start(row_copies(r))
        row_recv[r, pl.ds(lat, 1)] = row_send[r, pl.ds(lat, 1)]

    def backward(r):
        data = spectrum(row_recv[r], share)
        back = dot(t_back[0], data) + dot(t_back[1], data)
        now = x[r] + back.reshape(2, part, own)
        x[r] = now
        store_packed(tok_send, (r, slice(None)), now)
        start(tok_copies(r))
        tok_recv[r, pl.ds(ch, 1)] = tok_send[r, pl.ds(core, 1)]

    def token_piece(r, n):
        if n < chans:
            return tok_recv[r, n, 0:part].astype(F32)
        c = 2 * (n - chans)
        one = tok_recv[r, c, part : part + part // 2].astype(F32)
        two = tok_recv[r, c + 1, part : part + part // 2].astype(F32)
        rest = LANES // 2
        upper = jnp.concatenate((one[:, :rest], two[:, :rest]), -1)
        lower = jnp.concatenate((one[:, rest:], two[:, rest:]), -1)
        return jnp.concatenate((upper, lower), 0)

    def normalize(r):
        total, squares = 0.0, 0.0
        for n in range(wide // LANES):
            piece = token_piece(r, n)
            total = total + piece
            squares = squares + piece * piece
        mean = jnp.sum(total, -1, keepdims=True) / wide
        spread = jnp.sum(squares, -1, keepdims=True) / wide - mean * mean
        scaled = lax.rsqrt(spread + EPS)
        for n in range(wide // LANES):
            cut = slice(n * LANES, (n + 1) * LANES)
            normed = (token_piece(r, n) - mean) * scaled * par[0:1, cut] + par[1:2, cut]
            tokens[r % 2, 0:part, cut], tokens[r % 2, part : 2 * part, cut] = halves(normed)

    def project_up(r):
        for s, (weight, bias) in enumerate(((up, bias_send), (up_recv, bias_recv))):
            for lo in range(0, hid, 256):
                cut = slice(lo, lo + 256)
                both = dot(tokens[r % 2], weight[:, cut])
                pre = both[:part] + both[part:] + bias[0:1, cut]
                hidden[s, :, cut] = gelu(pre).astype(BF16)

    def project_down(r):
        for j in tuple(range(1, chips)) + (0,):
            first = pl.multiple_of(2 * own * lax.rem(chip + j, chips), LANES)
            cut = pl.ds(first, 2 * own)
            mixed = dot(hidden[0], down[:, cut]) + dot(hidden[1], down_recv[:, cut])
            for n in range(2):
                piece = mixed[:, n * own : (n + 1) * own]
                if j:
                    store_packed(mix_send, (r, j - 1, n), piece)
                else:
                    mix_full[r, n] = piece
            for q in (2 * j, 2 * j + 1):
                if q:
                    mix_copy(r, q).start()

    def residual(r):
        for h, piece in ((core, mix_full[r, pl.ds(core, 1)]), (1 - core, mix_pair[r][None])):
            for n in range(chips - 1):
                message = mix_recv[r, n, pl.ds(h, 1)]
                rest = unfold(message[:, part:])
                piece = piece + jnp.concatenate((message[:, :part].astype(F32), rest), -1)
            x[r, pl.ds(h, 1)] = x[r, pl.ds(h, 1)] + piece + shift[2:3]

    @pl.loop(0, STEPS)
    def _(index):
        for r in range(rows):
            forward(r)
        with jax.named_scope("wait_lon"):
            for r in range(rows):
                finish(lon_copies(r))
        with jax.named_scope("spectral"):
            pair = spectral()
        with jax.named_scope("unmix"):
            for r in range(rows):
                unmix(r, pair)
        for r in range(rows):
            with jax.named_scope("wait_row"):
                finish(row_copies(r))
            with jax.named_scope("backward"):
                backward(r)

        @pl.when(index == 0)
        def _():
            for each in loads[12:]:
                each.wait()
            finish(setup)
            pieces = [par_recv[c, 0:2, :LANES] for c in range(chans)]
            pieces += [par_recv[c, 0:2, LANES:] for c in range(chans)]
            par[...] = jnp.concatenate(pieces, -1)

        for r in range(rows):
            if r <= 1:
                with jax.named_scope("wait_tok"):
                    finish(tok_copies(r))
                with jax.named_scope("norm"):
                    normalize(r)
            with jax.named_scope("up"):
                project_up(r)
            if 1 <= r < rows - 1:
                with jax.named_scope("wait_tok"):
                    finish(tok_copies(r + 1))
            with jax.named_scope("down"):
                if 1 <= r < rows - 1:
                    normalize(r + 1)
                project_down(r)
        for r in range(rows):
            with jax.named_scope("wait_mix"):
                finish(mix_copies(r))
            with jax.named_scope("residual"):
                residual(r)

            @pl.when(index == STEPS - 1)
            def _():
                state[r, 0:near, 0] = x[r, 0, 0:near]
                state[r, near:width, 0] = x[r, 1, 0 : width - near]
                stores[r].start()

            @pl.when(index < STEPS - 1)
            def _():
                own_stats(r)
                start(stat_copies(r))

    for each in stores:
        each.wait()


def fused(
    lats,
    chans,
    state,
    norm_gains,
    channel_biases,
    filter_in,
    filter_in_bias,
    filter_out,
    filter_out_bias,
    up_weight,
    up_bias,
    down_weight,
):
    _, rows, width, own = state.shape
    part = -(--(-width // 2) // 16) * 16
    share = 2 * M // lats
    hid = up_weight.shape[1]
    tables = tuple(
        jnp.asarray(t) for t in fourier_tables(width, part, rows * lats, M, lats)
    )
    args = (
        state.transpose(1, 2, 0, 3),
        norm_gains,
        channel_biases,
        filter_in_bias,
        filter_out_bias,
        up_bias,
        filter_in,
        filter_out,
        up_weight,
        down_weight,
    ) + tables
    hbm = pl.BlockSpec(memory_space=pltpu.HBM)
    packed = share + share // 2
    spectrum = (rows, lats, packed, LANES)
    folded = part + part // 2
    peers = max(lats, chans)
    result = pl.pallas_call(
        functools.partial(rollout, lats, chans),
        out_shape=jax.ShapeDtypeStruct((rows, width, 1, own), F32),
        in_specs=[hbm] * 14,
        out_specs=hbm,
        scratch_shapes=[
            pltpu.VMEM((rows, width, 1, own), F32),
            pltpu.VMEM(norm_gains.shape, BF16),
            pltpu.VMEM(channel_biases.shape, BF16),
            pltpu.VMEM(filter_in_bias.shape, F32),
            pltpu.VMEM(filter_out_bias.shape, F32),
            pltpu.VMEM(up_bias.shape, BF16),
            pltpu.VMEM((rows, 2, part, own), F32),
            pltpu.VMEM((rows, 2, 2 * part), F32),
            pltpu.VMEM((rows, chans, 2, 2 * part), F32),
            pltpu.VMEM(spectrum, BF16),
            pltpu.VMEM((lats, rows, packed, LANES), BF16),
            pltpu.VMEM(spectrum, BF16),
            pltpu.VMEM(spectrum, BF16),
            pltpu.VMEM((rows, 2, folded, LANES), BF16),
            pltpu.VMEM((rows, chans, folded, LANES), BF16),
            pltpu.VMEM((rows, 2, part, own), F32),
            pltpu.VMEM((rows, chans // 2 - 1, 2, folded, LANES), BF16),
            pltpu.VMEM((rows, part, own), F32),
            pltpu.VMEM((rows, chans // 2 - 1, 2, folded, LANES), BF16),
            pltpu.VMEM((8, hid), F32),
            pltpu.VMEM((8, hid), F32),
            pltpu.VMEM((8, own), F32),
            pltpu.VMEM((chans, 8, own), F32),
            pltpu.VMEM((2, chans * own), F32),
            pltpu.VMEM(filter_in.shape, F32),
            pltpu.VMEM(filter_out.shape, F32),
            pltpu.VMEM((2, 2, own, own), BF16),
            pltpu.VMEM((2, 2, own, own), BF16),
            pltpu.VMEM((2, own), F32),
            pltpu.VMEM((2, own), F32),
            pltpu.VMEM(up_weight.shape, BF16),
            pltpu.VMEM(down_weight.shape, BF16),
            pltpu.VMEM(up_weight.shape, BF16),
            pltpu.VMEM(down_weight.shape, BF16),
        ]
        + [pltpu.VMEM(t.shape, BF16) for t in tables]
        + [
            pltpu.VMEM((2, 2 * part, chans * own), BF16),
            pltpu.VMEM((2, part, hid), BF16),
            pltpu.SemaphoreType.DMA((13 + 2 * chans,)),
            pltpu.SemaphoreType.DMA((6, max(rows, 3), peers)),
            pltpu.SemaphoreType.DMA((6, max(rows, 3), peers)),
        ],
        compiler_params=pltpu.CompilerParams(
            collective_id=0, has_side_effects=True, vmem_limit_bytes=60 * 1024 * 1024
        ),
    )(*args)
    return result.transpose(2, 0, 1, 3)


def dispatch(sizes, *args):
    lats, chans = sizes["lat"], sizes["ch"]
    own = args[0].shape[3]
    folds = own // LANES == 1 and 2 * (own % LANES) == LANES
    if folds and 2 * M // lats % 16 == 0 and chans > 2 and chans % 2 == 0:
        return fused(lats, chans, *args)
    return local(*args)


def solution(mesh):
    placed = (
        P(None, "lat", None, "ch"),
        P(None, "ch"),
        P(None, "ch"),
        P(None, "ch", None, None),
        P(None, "ch", None),
        P(None, "ch", None, None),
        P(None, "ch", None),
        P(None, "ch"),
        P("ch"),
        P("ch", None),
    )
    return jax.shard_map(
        functools.partial(dispatch, dict(mesh.shape)), mesh=mesh, in_specs=placed, out_specs=P(None, "lat", None, "ch"), check_vma=False
    )
```

```python
import functools
import math

import jax
import jax.numpy as jnp
from jax import lax
import numpy as np
from jax.experimental import pallas as pl
from jax.experimental.pallas import tpu as pltpu
from jax.sharding import PartitionSpec as P

D = 768
M = 64
STEPS = 4


EPS = 1e-05
SHRINK = 0.01
HIGH = lax.Precision.HIGHEST


def longitude_tables(width, modes):
    column = jnp.arange(width, dtype=jnp.int32)[:, None]
    order = jnp.arange(modes, dtype=jnp.int32)[None, :]
    angle = 2.0 * math.pi / width * (column * order % width).astype(jnp.float32)
    doubled = jnp.where(order == 0, 1.0, 2.0).astype(jnp.float32)
    return (jnp.cos(angle), jnp.sin(angle), jnp.cos(angle) * doubled, jnp.sin(angle) * doubled)


def latitude_tables(height):
    column = jnp.arange(height, dtype=jnp.int32)[:, None]
    order = jnp.arange(height, dtype=jnp.int32)[None, :]
    angle = 2.0 * math.pi / height * (column * order % height).astype(jnp.float32)
    return (jnp.cos(angle), jnp.sin(angle))


def layer_norm(values, gain, shift):
    mean = jnp.sum(values, -1, keepdims=True) / values.shape[-1]
    spread = jnp.sum(values * values, -1, keepdims=True) / values.shape[-1] - mean * mean
    return (values - mean) * lax.rsqrt(spread + EPS) * gain + shift


def soft_shrink(values):
    return jnp.where(
        values > SHRINK, values - SHRINK, jnp.where(values < -SHRINK, values + SHRINK, 0.0)
    )


def block_apply(left, matrix):
    return jnp.einsum("bkmnj,nji->bkmni", left, matrix, precision=HIGH)


def spectral_mlp(real_part, imag_part, filter_in, filter_in_bias, filter_out, filter_out_bias):
    shape = real_part.shape
    blocks = filter_in.shape[1]
    size = filter_in.shape[2]
    real_blocks = real_part.reshape(shape[:-1] + (blocks, size))
    imag_blocks = imag_part.reshape(shape[:-1] + (blocks, size))
    first_real = jax.nn.relu(
        block_apply(real_blocks, filter_in[0])
        - block_apply(imag_blocks, filter_in[1])
        + filter_in_bias[0]
    )
    first_imag = jax.nn.relu(
        block_apply(imag_blocks, filter_in[0])
        + block_apply(real_blocks, filter_in[1])
        + filter_in_bias[1]
    )
    second_real = (
        block_apply(first_real, filter_out[0])
        - block_apply(first_imag, filter_out[1])
        + filter_out_bias[0]
    )
    second_imag = (
        block_apply(first_imag, filter_out[0])
        + block_apply(first_real, filter_out[1])
        + filter_out_bias[1]
    )
    return (soft_shrink(second_real).reshape(shape), soft_shrink(second_imag).reshape(shape))


def local(
    state,
    norm_gains,
    channel_biases,
    filter_in,
    filter_in_bias,
    filter_out,
    filter_out_bias,
    up_weight,
    up_bias,
    down_weight,
):
    width = state.shape[2]
    height = state.shape[1] * lax.axis_size("lat")
    scale = 1.0 / math.sqrt(height * width)
    lon_cos, lon_sin, back_cos, back_sin = longitude_tables(width, M)
    lat_cos, lat_sin = latitude_tables(height)
    gains = norm_gains.astype(jnp.float32)
    shifts = channel_biases.astype(jnp.float32)
    full_up, full_gains, full_biases = (
        lax.all_gather(up_weight, "ch", axis=1, tiled=True),
        lax.all_gather(norm_gains, "ch", axis=1, tiled=True),
        lax.all_gather(channel_biases, "ch", axis=1, tiled=True),
    )
    full_down, full_up_bias = (
        lax.all_gather(down_weight, "ch", axis=0, tiled=True),
        lax.all_gather(up_bias, "ch", axis=0, tiled=True),
    )
    wide_gains = full_gains.astype(jnp.float32)
    wide_biases = full_biases.astype(jnp.float32)
    wide_up_bias = full_up_bias.astype(jnp.float32)
    values = state
    for step_index in range(STEPS):
        total, squares = lax.psum(
            (jnp.sum(values, -1, keepdims=True), jnp.sum(values * values, -1, keepdims=True)), "ch"
        )
        mean = total / D
        mean, spread = (mean, squares / D - mean * mean)
        normed = (values - mean) * lax.rsqrt(spread + EPS) * gains[0] + shifts[0]
        real_lon = jnp.einsum("bhwd,wm->bhmd", normed, lon_cos, precision=HIGH)
        imag_lon = -jnp.einsum("bhwd,wm->bhmd", normed, lon_sin, precision=HIGH)
        stacked = lax.all_to_all(
            jnp.stack((real_lon, imag_lon)), "lat", split_axis=3, concat_axis=2, tiled=True
        )
        spectral_real_lon = stacked[0]
        spectral_imag_lon = stacked[1]
        real_spec = (
            jnp.einsum("kh,bhmd->bkmd", lat_cos, spectral_real_lon, precision=HIGH)
            + jnp.einsum("kh,bhmd->bkmd", lat_sin, spectral_imag_lon, precision=HIGH)
        ) * scale
        imag_spec = (
            jnp.einsum("kh,bhmd->bkmd", lat_cos, spectral_imag_lon, precision=HIGH)
            - jnp.einsum("kh,bhmd->bkmd", lat_sin, spectral_real_lon, precision=HIGH)
        ) * scale
        out_real, out_imag = spectral_mlp(
            real_spec, imag_spec, filter_in, filter_in_bias, filter_out, filter_out_bias
        )
        real_rows = jnp.einsum("kh,bkmd->bhmd", lat_cos, out_real, precision=HIGH) - jnp.einsum(
            "kh,bkmd->bhmd", lat_sin, out_imag, precision=HIGH
        )
        imag_rows = jnp.einsum("kh,bkmd->bhmd", lat_cos, out_imag, precision=HIGH) + jnp.einsum(
            "kh,bkmd->bhmd", lat_sin, out_real, precision=HIGH
        )
        rows = lax.all_to_all(
            jnp.stack((real_rows, imag_rows)), "lat", split_axis=2, concat_axis=3, tiled=True
        )
        back = jnp.einsum("bhmd,wm->bhwd", rows[0], back_cos, precision=HIGH) - jnp.einsum(
            "bhmd,wm->bhwd", rows[1], back_sin, precision=HIGH
        )
        values = values + back * scale + normed
        owned = lax.all_to_all(values, "ch", split_axis=2, concat_axis=3, tiled=True)
        normed_two = layer_norm(owned, wide_gains[1], wide_biases[1]).astype(jnp.bfloat16)
        flat = normed_two.reshape(-1, normed_two.shape[-1])
        pre = jnp.dot(flat, full_up, preferred_element_type=jnp.float32) + wide_up_bias
        hidden = jax.nn.gelu(pre, approximate=False).astype(jnp.bfloat16)
        mixed = jnp.dot(hidden, full_down, preferred_element_type=jnp.float32) + wide_biases[2]
        values = values + lax.all_to_all(
            mixed.reshape(owned.shape), "ch", split_axis=3, concat_axis=2, tiled=True
        )
    return values


F32 = jnp.float32
BF16 = jnp.bfloat16
MESH = pl.DeviceIdType.MESH


def split_table(table):
    high = np.asarray(table, np.float32).astype(jnp.bfloat16)
    low = (table - high.astype(np.float64)).astype(np.float32).astype(jnp.bfloat16)
    return np.stack((high, low))


def fourier_tables(width, part, height, modes, owners):
    scale = 1.0 / math.sqrt(height * width)
    share = modes // owners
    rows = height // owners
    half = -(-width // 2)
    token = np.arange(width)
    place = token // half * part + token % half
    order = np.arange(modes).reshape(owners, share)
    angle = 2.0 * np.pi / width * (order[:, :, None] * token % width)
    forward = np.zeros((owners, 2, share, 2 * part))
    forward[:, 0, :, place] = np.moveaxis(np.cos(angle), -1, 0)
    forward[:, 1, :, place] = np.moveaxis(-np.sin(angle), -1, 0)
    doubled = np.where(order == 0, 1.0, 2.0)[:, None, :, None] * scale
    backward = (forward * doubled).reshape(2 * modes, 2 * part).T
    forward = forward.reshape(2 * modes, 2 * part)
    turns = np.arange(height)
    turn = 2.0 * np.pi / height * (turns[:, None] * turns[None, :] % height)
    cos, sin, eye = np.cos(turn), np.sin(turn), np.eye(share)
    mix = np.array([[cos, sin], [-sin, cos]])
    size = 2 * height * share
    lat = np.einsum("abkh,mn->akmhbn", mix, eye).reshape(size, size) * scale
    unmix = np.array([[cos, -sin], [sin, cos]])
    back = np.einsum("bahk,mn->hbmakn", unmix, eye)
    back = back.reshape((owners, rows) + back.shape[1:]).swapaxes(0, 1).reshape(size, size)
    return tuple(split_table(t) for t in (forward, lat, back, backward))


def dot(left, right):
    return jnp.dot(left, right, preferred_element_type=F32)


def halves(values):
    high = values.astype(BF16)
    return high, (values - high.astype(F32)).astype(BF16)


def dot3(left, right):
    return dot(left[0], right[0]) + dot(left[1], right[0]) + dot(left[0], right[1])


def gelu(values):
    return 0.5 * values * (1.0 + lax.erf(values * (1.0 / math.sqrt(2.0))))


def flip(index, bits):
    bit, moved = 1, index
    while bit <= bits:
        if bits & bit:
            moved = moved + bit - 2 * bit * lax.rem(lax.div(index, bit), 2)
        bit *= 2
    return moved


LANES = 128


def pack(values):
    rows = values.shape[-2] // 2
    rest = values[..., LANES:]
    folded = jnp.concatenate((rest[..., :rows, :], rest[..., rows:, :]), -1)
    return values[..., :LANES].astype(BF16), folded.astype(BF16)


def unfold(folded):
    values = folded.astype(F32)
    return jnp.concatenate((values[..., : LANES // 2], values[..., LANES // 2 :]), -2)


def store_packed(target, where, values):
    rows = values.shape[-2]
    full, folded = pack(values)
    target[where + (slice(0, rows),)] = full
    target[where + (slice(rows, rows + rows // 2),)] = folded


STAT, LON, ROW, TOK, MIX, SETUP = range(6)


def rollout(
    lats,
    chans,
    state_hbm,
    gains_hbm,
    shifts_hbm,
    fin_bias_hbm,
    fout_bias_hbm,
    up_bias_hbm,
    fin_hbm,
    fout_hbm,
    up_hbm,
    down_hbm,
    t_lon_hbm,
    t_lat_hbm,
    t_rows_hbm,
    t_back_hbm,
    out_hbm,
    state,
    gains,
    shifts,
    fin_bias,
    fout_bias,
    up_bias,
    x,
    stat_send,
    stat_recv,
    lon_send,
    lon_recv,
    row_send,
    row_recv,
    tok_send,
    tok_recv,
    mix_full,
    mix_send,
    mix_pair,
    mix_recv,
    bias_send,
    bias_recv,
    par_send,
    par_recv,
    par,
    fin_raw,
    fout_raw,
    fin,
    fout,
    fin_b,
    fout_b,
    up,
    down,
    up_recv,
    down_recv,
    t_lon,
    t_lat,
    t_rows,
    t_back,
    tokens,
    hidden,
    load_sem,
    send_sem,
    recv_sem,
):
    lat, ch = lax.axis_index("lat"), lax.axis_index("ch")
    core, chip = lax.rem(ch, 2), lax.div(ch, 2)
    chips = chans // 2
    rows, width, _, own = state.shape
    part = x.shape[2]
    near = -(-width // 2)
    wide = chans * own
    hid = up.shape[1]
    spread_modes = t_lon.shape[1]

    def chan(q):
        return 2 * lax.rem(chip + q // 2, chips) + (core if q % 2 == 0 else 1 - core)

    def half_of(q):
        return core if q % 2 == 0 else 1 - core

    up_rows = []
    for c in range(chans):
        up_rows.append((pl.ds(c * own, LANES), pl.ds(c * LANES, LANES)))
        rest = own - LANES
        up_rows.append((pl.ds(c * own + LANES, rest), pl.ds(chans * LANES + c * rest, rest)))

    lat_order = sorted(range(1, lats), key=lambda k: -4 * (2 * k // lats) - 2 * (k % 2) - k / lats)
    ch_order = tuple(range(2, chans)) + (1,)

    loads = [
        pltpu.make_async_copy(source, target, load_sem.at[n])
        for n, (source, target) in enumerate(
            (
                (state_hbm, state),
                (gains_hbm, gains),
                (shifts_hbm, shifts),
                (up_bias_hbm, up_bias),
                (fin_bias_hbm, fin_bias),
                (fout_bias_hbm, fout_bias),
                (fin_hbm, fin_raw),
                (fout_hbm, fout_raw),
                (t_lon_hbm, t_lon),
                (t_lat_hbm, t_lat),
                (t_rows_hbm, t_rows),
                (t_back_hbm, t_back),
                (down_hbm, down),
            )
            + tuple((up_hbm.at[source], up.at[target]) for source, target in up_rows)
        )
    ]
    for each in loads:
        each.start()
    stores = [
        pltpu.make_async_copy(state.at[r], out_hbm.at[r], load_sem.at[r]) for r in range(rows)
    ]

    barrier = pltpu.get_barrier_semaphore()
    for k in lat_order:
        pl.semaphore_signal(barrier, inc=1, device_id={"lat": flip(lat, k)}, device_id_type=MESH)
    for q in ch_order:
        pl.semaphore_signal(barrier, inc=1, device_id={"ch": chan(q)}, device_id_type=MESH)

    def copy(kind, r, k, source, target, device):
        return pltpu.make_async_remote_copy(
            src_ref=source,
            dst_ref=target,
            send_sem=send_sem.at[kind, r, k],
            recv_sem=recv_sem.at[kind, r, k],
            device_id=device,
            device_id_type=MESH,
        )

    def stat_copies(r):
        return [
            copy(STAT, r, q, stat_send.at[r], stat_recv.at[r, ch], {"ch": chan(q)})
            for q in ch_order
        ]

    def lon_copies(r):
        return [
            copy(LON, r, k, lon_send.at[r, flip(lat, k)], lon_recv.at[lat, r], {"lat": flip(lat, k)})
            for k in lat_order
        ]

    def row_copies(r):
        return [
            copy(ROW, r, k, row_send.at[r, flip(lat, k)], row_recv.at[r, lat], {"lat": flip(lat, k)})
            for k in lat_order
        ]

    def tok_copies(r):
        return [
            copy(TOK, r, q, tok_send.at[r, half_of(q)], tok_recv.at[r, ch], {"ch": chan(q)})
            for q in ch_order
        ]

    def mix_copy(r, q):
        if q == 1:
            return copy(MIX, r, q, mix_full.at[r, 1 - core], mix_pair.at[r], {"ch": chan(q)})
        n = q // 2 - 1
        source = mix_send.at[r, n, half_of(q)]
        return copy(MIX, r, q, source, mix_recv.at[r, n, core], {"ch": chan(q)})

    def mix_copies(r):
        return [mix_copy(r, q) for q in ch_order]

    def start(copies):
        for each in copies:
            each.start()

    def finish(copies):
        for each in copies:
            each.wait()

    x[...] = jnp.zeros_like(x)
    loads[0].wait()
    for r in range(rows):
        x[r, 0, 0:near] = state[r, 0:near, 0]
        x[r, 1, 0 : width - near] = state[r, near:width, 0]
    ones = jnp.ones((8, own), BF16)
    which = lax.broadcasted_iota(jnp.int32, (8, 2 * part), 0)

    def row_sums(values):
        dims = (((1,), (1,)), ((), ()))
        high, low = halves(values)
        return lax.dot_general(
            ones, high, dims, preferred_element_type=F32
        ) + lax.dot_general(ones, low, dims, preferred_element_type=F32)

    def own_stats(r):
        values = x[r].reshape(2 * part, own)
        sums = jnp.where(which == 0, row_sums(values), row_sums(values * values))
        stat_send[r] = sums[0:2]
        stat_recv[r, pl.ds(ch, 1)] = sums[None, 0:2]

    def take_stats(r):
        with jax.named_scope("wait_stat"):
            finish(stat_copies(r))
        total = stat_recv[r, 0]
        for c in range(1, chans):
            total = total + stat_recv[r, c]
        mean = total[0:1] / wide
        scaled = lax.rsqrt(total[1:2] / wide - mean * mean + EPS)
        both = jnp.transpose(jnp.where(which == 0, mean, scaled))
        return both[:, 0:1], both[:, 1:2]

    for r in range(rows):
        own_stats(r)
    pl.semaphore_wait(barrier, lats + chans - 2)
    for r in range(rows):
        start(stat_copies(r))
    for each in loads[1:4]:
        each.wait()
    gain = gains[...].astype(F32)
    shift = shifts[...].astype(F32)
    par_send[...] = jnp.concatenate((gain[1:2], shift[1:2], jnp.zeros((6, own), F32)), 0)
    par_recv[pl.ds(ch, 1)] = par_send[...][None]
    bias_send[...] = jnp.broadcast_to(up_bias[...].astype(F32)[None], bias_send.shape)
    partner = {"ch": chan(1)}
    setup = [
        copy(SETUP, 0, 0, down_hbm, down_recv, partner),
        copy(SETUP, 0, 1, bias_send, bias_recv, partner),
    ]
    for n, (source, target) in enumerate(up_rows):
        setup.append(
            copy(SETUP, 1 + n // chans, n % chans, up_hbm.at[source], up_recv.at[target], partner)
        )
    for n, q in enumerate(ch_order):
        setup.append(copy(SETUP, 0, 2 + n, par_send, par_recv.at[ch], {"ch": chan(q)}))
    start(setup)
    for each in loads[4:8]:
        each.wait()
    blocks, size = fin_raw.shape[1], fin_raw.shape[2]
    line = lax.broadcasted_iota(jnp.int32, (size, own), 0)
    lane = lax.broadcasted_iota(jnp.int32, (size, own), 1)
    for raw, target, bias, bias_target in (
        (fin_raw, fin, fin_bias, fin_b),
        (fout_raw, fout, fout_bias, fout_b),
    ):
        placed = 0.0
        for n in range(blocks):
            shifted = jnp.where(lane == line + n * size, 1.0, 0.0)
            select = shifted.astype(BF16)
            for p in range(2):
                high, low = halves(raw[p, n])
                target[p, 0, n * size : (n + 1) * size] = dot(high, select).astype(BF16)
                target[p, 1, n * size : (n + 1) * size] = dot(low, select).astype(BF16)
            placed = placed + jnp.dot(
                bias[:, n, :], shifted, precision=HIGH, preferred_element_type=F32
            )
        bias_target[...] = placed
    for each in loads[8:12]:
        each.wait()

    def complex_apply(pair, weights, bias):
        split = pair.shape[0] // 2
        pair = halves(pair)
        one = dot3(pair, (weights[0, 0], weights[0, 1]))
        two = dot3(pair, (weights[1, 0], weights[1, 1]))
        return (
            one[:split] - two[split:] + bias[0:1, :],
            one[split:] + two[:split] + bias[1:2, :],
        )

    def spectrum(messages, count):
        full = messages[..., :count, :]
        rest = unfold(messages[..., count:, :]).astype(BF16)
        return jnp.concatenate((full, rest), -1).reshape(-1, own)

    share = spread_modes // lats

    def forward(r):
        with jax.named_scope("forward"):
            mean, scaled = take_stats(r)
            now = x[r].reshape(2 * part, own)
            normed = (now - mean) * scaled * gain[0:1] + shift[0:1]
            x[r] = (now + normed).reshape(2, part, own)
            spectra = dot3((t_lon[0], t_lon[1]), halves(normed))
            store_packed(lon_send, (r, slice(None)), spectra.reshape(lats, share, own))
            start(lon_copies(r))
            lon_recv[pl.ds(lat, 1), r] = lon_send[r, pl.ds(lat, 1)]

    def spectral():
        data = spectrum(lon_recv[...], share)
        size = t_lat.shape[1] // 4
        spec = []
        for n in range(4):
            cut = slice(n * size, (n + 1) * size)
            spec.append(dot(t_lat[0, cut], data) + dot(t_lat[1, cut], data))
        spec = jnp.concatenate(spec, 0)
        real, imag = complex_apply(spec, fin, fin_b)
        pair = jnp.concatenate((jnp.maximum(real, 0.0), jnp.maximum(imag, 0.0)), 0)
        real, imag = complex_apply(pair, fout, fout_b)
        return halves(jnp.concatenate((soft_shrink(real), soft_shrink(imag)), 0))

    def unmix(r, pair):
        count = spread_modes // 2
        for n in range(2):
            first = r * spread_modes + n * count
            cut = slice(first, first + count)
            back = dot3((t_rows[0, cut], t_rows[1, cut]), pair)
            where = (r, slice(n * lats // 2, (n + 1) * lats // 2))
            store_packed(row_send, where, back.reshape(lats // 2, share, own))
        start(row_copies(r))
        row_recv[r, pl.ds(lat, 1)] = row_send[r, pl.ds(lat, 1)]

    def backward(r):
        data = spectrum(row_recv[r], share)
        back = dot(t_back[0], data) + dot(t_back[1], data)
        now = x[r] + back.reshape(2, part, own)
        x[r] = now
        store_packed(tok_send, (r, slice(None)), now)
        start(tok_copies(r))
        tok_recv[r, pl.ds(ch, 1)] = tok_send[r, pl.ds(core, 1)]

    def token_piece(r, n):
        if n < chans:
            return tok_recv[r, n, 0:part].astype(F32)
        c = 2 * (n - chans)
        one = tok_recv[r, c, part : part + part // 2].astype(F32)
        two = tok_recv[r, c + 1, part : part + part // 2].astype(F32)
        rest = LANES // 2
        upper = jnp.concatenate((one[:, :rest], two[:, :rest]), -1)
        lower = jnp.concatenate((one[:, rest:], two[:, rest:]), -1)
        return jnp.concatenate((upper, lower), 0)

    def normalize(r):
        total, squares = 0.0, 0.0
        for n in range(wide // LANES):
            piece = token_piece(r, n)
            total = total + piece
            squares = squares + piece * piece
        mean = jnp.sum(total, -1, keepdims=True) / wide
        spread = jnp.sum(squares, -1, keepdims=True) / wide - mean * mean
        scaled = lax.rsqrt(spread + EPS)
        for n in range(wide // LANES):
            cut = slice(n * LANES, (n + 1) * LANES)
            normed = (token_piece(r, n) - mean) * scaled * par[0:1, cut] + par[1:2, cut]
            tokens[r % 2, 0:part, cut], tokens[r % 2, part : 2 * part, cut] = halves(normed)

    def project_up(r):
        for s, (weight, bias) in enumerate(((up, bias_send), (up_recv, bias_recv))):
            for lo in range(0, hid, 256):
                cut = slice(lo, lo + 256)
                both = dot(tokens[r % 2], weight[:, cut])
                pre = both[:part] + both[part:] + bias[0:1, cut]
                hidden[s, :, cut] = gelu(pre).astype(BF16)

    def project_down(r):
        for j in tuple(range(1, chips)) + (0,):
            first = pl.multiple_of(2 * own * lax.rem(chip + j, chips), LANES)
            cut = pl.ds(first, 2 * own)
            mixed = dot(hidden[0], down[:, cut]) + dot(hidden[1], down_recv[:, cut])
            for n in range(2):
                piece = mixed[:, n * own : (n + 1) * own]
                if j:
                    store_packed(mix_send, (r, j - 1, n), piece)
                else:
                    mix_full[r, n] = piece
            for q in (2 * j, 2 * j + 1):
                if q:
                    mix_copy(r, q).start()

    def residual(r):
        for h, piece in ((core, mix_full[r, pl.ds(core, 1)]), (1 - core, mix_pair[r][None])):
            for n in range(chips - 1):
                message = mix_recv[r, n, pl.ds(h, 1)]
                rest = unfold(message[:, part:])
                piece = piece + jnp.concatenate((message[:, :part].astype(F32), rest), -1)
            x[r, pl.ds(h, 1)] = x[r, pl.ds(h, 1)] + piece + shift[2:3]

    @pl.loop(0, STEPS)
    def _(index):
        for r in range(rows):
            forward(r)
        with jax.named_scope("wait_lon"):
            for r in range(rows):
                finish(lon_copies(r))
        with jax.named_scope("spectral"):
            pair = spectral()
        with jax.named_scope("unmix"):
            for r in range(rows):
                unmix(r, pair)
        for r in range(rows):
            with jax.named_scope("wait_row"):
                finish(row_copies(r))
            with jax.named_scope("backward"):
                backward(r)

        @pl.when(index == 0)
        def _():
            for each in loads[12:]:
                each.wait()
            finish(setup)
            pieces = [par_recv[c, 0:2, :LANES] for c in range(chans)]
            pieces += [par_recv[c, 0:2, LANES:] for c in range(chans)]
            par[...] = jnp.concatenate(pieces, -1)

        for r in range(rows):
            if r <= 1:
                with jax.named_scope("wait_tok"):
                    finish(tok_copies(r))
                with jax.named_scope("norm"):
                    normalize(r)
            with jax.named_scope("up"):
                project_up(r)
            if 1 <= r < rows - 1:
                with jax.named_scope("wait_tok"):
                    finish(tok_copies(r + 1))
            with jax.named_scope("down"):
                if 1 <= r < rows - 1:
                    normalize(r + 1)
                project_down(r)
        for r in range(rows):
            with jax.named_scope("wait_mix"):
                finish(mix_copies(r))
            with jax.named_scope("residual"):
                residual(r)

            @pl.when(index == STEPS - 1)
            def _():
                state[r, 0:near, 0] = x[r, 0, 0:near]
                state[r, near:width, 0] = x[r, 1, 0 : width - near]
                stores[r].start()

            @pl.when(index < STEPS - 1)
            def _():
                own_stats(r)
                start(stat_copies(r))

    for each in stores:
        each.wait()


def hand_over(source, target, held, read_sem, write_sem):
    rows = source.shape[0]
    reads = [pltpu.make_async_copy(source.at[r], held.at[r], read_sem.at[r]) for r in range(rows)]
    writes = [pltpu.make_async_copy(held.at[r], target.at[r], write_sem.at[r]) for r in range(rows)]
    for each in reads:
        each.start()
    for read, write in zip(reads, writes):
        read.wait()
        write.start()
    for each in writes:
        each.wait()


def fused(
    lats,
    chans,
    state,
    norm_gains,
    channel_biases,
    filter_in,
    filter_in_bias,
    filter_out,
    filter_out_bias,
    up_weight,
    up_bias,
    down_weight,
):
    _, rows, width, own = state.shape
    part = -(--(-width // 2) // 16) * 16
    share = 2 * M // lats
    hid = up_weight.shape[1]
    tables = tuple(
        jnp.asarray(t) for t in fourier_tables(width, part, rows * lats, M, lats)
    )
    args = (
        state.transpose(1, 2, 0, 3),
        norm_gains,
        channel_biases,
        filter_in_bias,
        filter_out_bias,
        up_bias,
        filter_in,
        filter_out,
        up_weight,
        down_weight,
    ) + tables
    hbm = pl.BlockSpec(memory_space=pltpu.HBM)
    packed = share + share // 2
    spectrum = (rows, lats, packed, LANES)
    folded = part + part // 2
    peers = max(lats, chans)
    result = pl.pallas_call(
        functools.partial(rollout, lats, chans),
        out_shape=jax.ShapeDtypeStruct((rows, width, 1, own), F32),
        in_specs=[hbm] * 14,
        out_specs=hbm,
        scratch_shapes=[
            pltpu.VMEM((rows, width, 1, own), F32),
            pltpu.VMEM(norm_gains.shape, BF16),
            pltpu.VMEM(channel_biases.shape, BF16),
            pltpu.VMEM(filter_in_bias.shape, F32),
            pltpu.VMEM(filter_out_bias.shape, F32),
            pltpu.VMEM(up_bias.shape, BF16),
            pltpu.VMEM((rows, 2, part, own), F32),
            pltpu.VMEM((rows, 2, 2 * part), F32),
            pltpu.VMEM((rows, chans, 2, 2 * part), F32),
            pltpu.VMEM(spectrum, BF16),
            pltpu.VMEM((lats, rows, packed, LANES), BF16),
            pltpu.VMEM(spectrum, BF16),
            pltpu.VMEM(spectrum, BF16),
            pltpu.VMEM((rows, 2, folded, LANES), BF16),
            pltpu.VMEM((rows, chans, folded, LANES), BF16),
            pltpu.VMEM((rows, 2, part, own), F32),
            pltpu.VMEM((rows, chans // 2 - 1, 2, folded, LANES), BF16),
            pltpu.VMEM((rows, part, own), F32),
            pltpu.VMEM((rows, chans // 2 - 1, 2, folded, LANES), BF16),
            pltpu.VMEM((8, hid), F32),
            pltpu.VMEM((8, hid), F32),
            pltpu.VMEM((8, own), F32),
            pltpu.VMEM((chans, 8, own), F32),
            pltpu.VMEM((2, chans * own), F32),
            pltpu.VMEM(filter_in.shape, F32),
            pltpu.VMEM(filter_out.shape, F32),
            pltpu.VMEM((2, 2, own, own), BF16),
            pltpu.VMEM((2, 2, own, own), BF16),
            pltpu.VMEM((2, own), F32),
            pltpu.VMEM((2, own), F32),
            pltpu.VMEM(up_weight.shape, BF16),
            pltpu.VMEM(down_weight.shape, BF16),
            pltpu.VMEM(up_weight.shape, BF16),
            pltpu.VMEM(down_weight.shape, BF16),
        ]
        + [pltpu.VMEM(t.shape, BF16) for t in tables]
        + [
            pltpu.VMEM((2, 2 * part, chans * own), BF16),
            pltpu.VMEM((2, part, hid), BF16),
            pltpu.SemaphoreType.DMA((13 + 2 * chans,)),
            pltpu.SemaphoreType.DMA((6, max(rows, 3), peers)),
            pltpu.SemaphoreType.DMA((6, max(rows, 3), peers)),
        ],
        compiler_params=pltpu.CompilerParams(
            collective_id=0, has_side_effects=True, vmem_limit_bytes=60 * 1024 * 1024
        ),
    )(*args)
    result = pl.pallas_call(
        hand_over,
        out_shape=jax.ShapeDtypeStruct(result.shape, F32),
        in_specs=[hbm],
        out_specs=hbm,
        scratch_shapes=[
            pltpu.VMEM(result.shape, F32),
            pltpu.SemaphoreType.DMA((rows,)),
            pltpu.SemaphoreType.DMA((rows,)),
        ],
        compiler_params=pltpu.CompilerParams(vmem_limit_bytes=60 * 1024 * 1024),
    )(result)
    return result.transpose(2, 0, 1, 3)


def dispatch(sizes, *args):
    lats, chans = sizes["lat"], sizes["ch"]
    own = args[0].shape[3]
    folds = own // LANES == 1 and 2 * (own % LANES) == LANES
    if folds and 2 * M // lats % 16 == 0 and chans > 2 and chans % 2 == 0:
        return fused(lats, chans, *args)
    return local(*args)


def solution(mesh):
    placed = (
        P(None, "lat", None, "ch"),
        P(None, "ch"),
        P(None, "ch"),
        P(None, "ch", None, None),
        P(None, "ch", None),
        P(None, "ch", None, None),
        P(None, "ch", None),
        P(None, "ch"),
        P("ch"),
        P("ch", None),
    )
    return jax.shard_map(
        functools.partial(dispatch, dict(mesh.shape)), mesh=mesh, in_specs=placed, out_specs=P(None, "lat", None, "ch"), check_vma=False
    )
```

```python
import functools
import math

import jax
import jax.numpy as jnp
from jax import lax
import numpy as np
from jax.experimental import pallas as pl
from jax.experimental.pallas import tpu as pltpu
from jax.sharding import PartitionSpec as P

D = 768
M = 64
STEPS = 4


EPS = 1e-05
SHRINK = 0.01
HIGH = lax.Precision.HIGHEST


def longitude_tables(width, modes):
    column = jnp.arange(width, dtype=jnp.int32)[:, None]
    order = jnp.arange(modes, dtype=jnp.int32)[None, :]
    angle = 2.0 * math.pi / width * (column * order % width).astype(jnp.float32)
    doubled = jnp.where(order == 0, 1.0, 2.0).astype(jnp.float32)
    return (jnp.cos(angle), jnp.sin(angle), jnp.cos(angle) * doubled, jnp.sin(angle) * doubled)


def latitude_tables(height):
    column = jnp.arange(height, dtype=jnp.int32)[:, None]
    order = jnp.arange(height, dtype=jnp.int32)[None, :]
    angle = 2.0 * math.pi / height * (column * order % height).astype(jnp.float32)
    return (jnp.cos(angle), jnp.sin(angle))


def layer_norm(values, gain, shift):
    mean = jnp.sum(values, -1, keepdims=True) / values.shape[-1]
    spread = jnp.sum(values * values, -1, keepdims=True) / values.shape[-1] - mean * mean
    return (values - mean) * lax.rsqrt(spread + EPS) * gain + shift


def soft_shrink(values):
    return jnp.where(
        values > SHRINK, values - SHRINK, jnp.where(values < -SHRINK, values + SHRINK, 0.0)
    )


def block_apply(left, matrix):
    return jnp.einsum("bkmnj,nji->bkmni", left, matrix, precision=HIGH)


def spectral_mlp(real_part, imag_part, filter_in, filter_in_bias, filter_out, filter_out_bias):
    shape = real_part.shape
    blocks = filter_in.shape[1]
    size = filter_in.shape[2]
    real_blocks = real_part.reshape(shape[:-1] + (blocks, size))
    imag_blocks = imag_part.reshape(shape[:-1] + (blocks, size))
    first_real = jax.nn.relu(
        block_apply(real_blocks, filter_in[0])
        - block_apply(imag_blocks, filter_in[1])
        + filter_in_bias[0]
    )
    first_imag = jax.nn.relu(
        block_apply(imag_blocks, filter_in[0])
        + block_apply(real_blocks, filter_in[1])
        + filter_in_bias[1]
    )
    second_real = (
        block_apply(first_real, filter_out[0])
        - block_apply(first_imag, filter_out[1])
        + filter_out_bias[0]
    )
    second_imag = (
        block_apply(first_imag, filter_out[0])
        + block_apply(first_real, filter_out[1])
        + filter_out_bias[1]
    )
    return (soft_shrink(second_real).reshape(shape), soft_shrink(second_imag).reshape(shape))


def local(
    state,
    norm_gains,
    channel_biases,
    filter_in,
    filter_in_bias,
    filter_out,
    filter_out_bias,
    up_weight,
    up_bias,
    down_weight,
):
    width = state.shape[2]
    height = state.shape[1] * lax.axis_size("lat")
    scale = 1.0 / math.sqrt(height * width)
    lon_cos, lon_sin, back_cos, back_sin = longitude_tables(width, M)
    lat_cos, lat_sin = latitude_tables(height)
    gains = norm_gains.astype(jnp.float32)
    shifts = channel_biases.astype(jnp.float32)
    full_up, full_gains, full_biases = (
        lax.all_gather(up_weight, "ch", axis=1, tiled=True),
        lax.all_gather(norm_gains, "ch", axis=1, tiled=True),
        lax.all_gather(channel_biases, "ch", axis=1, tiled=True),
    )
    full_down, full_up_bias = (
        lax.all_gather(down_weight, "ch", axis=0, tiled=True),
        lax.all_gather(up_bias, "ch", axis=0, tiled=True),
    )
    wide_gains = full_gains.astype(jnp.float32)
    wide_biases = full_biases.astype(jnp.float32)
    wide_up_bias = full_up_bias.astype(jnp.float32)
    values = state
    for step_index in range(STEPS):
        total, squares = lax.psum(
            (jnp.sum(values, -1, keepdims=True), jnp.sum(values * values, -1, keepdims=True)), "ch"
        )
        mean = total / D
        mean, spread = (mean, squares / D - mean * mean)
        normed = (values - mean) * lax.rsqrt(spread + EPS) * gains[0] + shifts[0]
        real_lon = jnp.einsum("bhwd,wm->bhmd", normed, lon_cos, precision=HIGH)
        imag_lon = -jnp.einsum("bhwd,wm->bhmd", normed, lon_sin, precision=HIGH)
        stacked = lax.all_to_all(
            jnp.stack((real_lon, imag_lon)), "lat", split_axis=3, concat_axis=2, tiled=True
        )
        spectral_real_lon = stacked[0]
        spectral_imag_lon = stacked[1]
        real_spec = (
            jnp.einsum("kh,bhmd->bkmd", lat_cos, spectral_real_lon, precision=HIGH)
            + jnp.einsum("kh,bhmd->bkmd", lat_sin, spectral_imag_lon, precision=HIGH)
        ) * scale
        imag_spec = (
            jnp.einsum("kh,bhmd->bkmd", lat_cos, spectral_imag_lon, precision=HIGH)
            - jnp.einsum("kh,bhmd->bkmd", lat_sin, spectral_real_lon, precision=HIGH)
        ) * scale
        out_real, out_imag = spectral_mlp(
            real_spec, imag_spec, filter_in, filter_in_bias, filter_out, filter_out_bias
        )
        real_rows = jnp.einsum("kh,bkmd->bhmd", lat_cos, out_real, precision=HIGH) - jnp.einsum(
            "kh,bkmd->bhmd", lat_sin, out_imag, precision=HIGH
        )
        imag_rows = jnp.einsum("kh,bkmd->bhmd", lat_cos, out_imag, precision=HIGH) + jnp.einsum(
            "kh,bkmd->bhmd", lat_sin, out_real, precision=HIGH
        )
        rows = lax.all_to_all(
            jnp.stack((real_rows, imag_rows)), "lat", split_axis=2, concat_axis=3, tiled=True
        )
        back = jnp.einsum("bhmd,wm->bhwd", rows[0], back_cos, precision=HIGH) - jnp.einsum(
            "bhmd,wm->bhwd", rows[1], back_sin, precision=HIGH
        )
        values = values + back * scale + normed
        owned = lax.all_to_all(values, "ch", split_axis=2, concat_axis=3, tiled=True)
        normed_two = layer_norm(owned, wide_gains[1], wide_biases[1]).astype(jnp.bfloat16)
        flat = normed_two.reshape(-1, normed_two.shape[-1])
        pre = jnp.dot(flat, full_up, preferred_element_type=jnp.float32) + wide_up_bias
        hidden = jax.nn.gelu(pre, approximate=False).astype(jnp.bfloat16)
        mixed = jnp.dot(hidden, full_down, preferred_element_type=jnp.float32) + wide_biases[2]
        values = values + lax.all_to_all(
            mixed.reshape(owned.shape), "ch", split_axis=3, concat_axis=2, tiled=True
        )
    return values


F32 = jnp.float32
BF16 = jnp.bfloat16
MESH = pl.DeviceIdType.MESH


def split_table(table):
    high = np.asarray(table, np.float32).astype(jnp.bfloat16)
    low = (table - high.astype(np.float64)).astype(np.float32).astype(jnp.bfloat16)
    return np.stack((high, low))


def fourier_tables(width, part, height, modes, owners):
    scale = 1.0 / math.sqrt(height * width)
    share = modes // owners
    rows = height // owners
    half = -(-width // 2)
    token = np.arange(width)
    place = token // half * part + token % half
    order = np.arange(modes).reshape(owners, share)
    angle = 2.0 * np.pi / width * (order[:, :, None] * token % width)
    forward = np.zeros((owners, 2, share, 2 * part))
    forward[:, 0, :, place] = np.moveaxis(np.cos(angle), -1, 0)
    forward[:, 1, :, place] = np.moveaxis(-np.sin(angle), -1, 0)
    doubled = np.where(order == 0, 1.0, 2.0)[:, None, :, None] * scale
    backward = (forward * doubled).reshape(2 * modes, 2 * part).T
    forward = forward.reshape(2 * modes, 2 * part)
    turns = np.arange(height)
    turn = 2.0 * np.pi / height * (turns[:, None] * turns[None, :] % height)
    cos, sin, eye = np.cos(turn), np.sin(turn), np.eye(share)
    mix = np.array([[cos, sin], [-sin, cos]])
    size = 2 * height * share
    lat = np.einsum("abkh,mn->akmhbn", mix, eye).reshape(size, size) * scale
    unmix = np.array([[cos, -sin], [sin, cos]])
    back = np.einsum("bahk,mn->hbmakn", unmix, eye)
    back = back.reshape((owners, rows) + back.shape[1:]).swapaxes(0, 1).reshape(size, size)
    return tuple(split_table(t) for t in (forward, lat, back, backward))


def dot(left, right):
    return jnp.dot(left, right, preferred_element_type=F32)


def halves(values):
    high = values.astype(BF16)
    return high, (values - high.astype(F32)).astype(BF16)


def dot3(left, right):
    return dot(left[0], right[0]) + dot(left[1], right[0]) + dot(left[0], right[1])


def gelu(values):
    return 0.5 * values * (1.0 + lax.erf(values * (1.0 / math.sqrt(2.0))))


def flip(index, bits):
    bit, moved = 1, index
    while bit <= bits:
        if bits & bit:
            moved = moved + bit - 2 * bit * lax.rem(lax.div(index, bit), 2)
        bit *= 2
    return moved


LANES = 128


def pack(values):
    rows = values.shape[-2] // 2
    rest = values[..., LANES:]
    folded = jnp.concatenate((rest[..., :rows, :], rest[..., rows:, :]), -1)
    return values[..., :LANES].astype(BF16), folded.astype(BF16)


def unfold(folded):
    values = folded.astype(F32)
    return jnp.concatenate((values[..., : LANES // 2], values[..., LANES // 2 :]), -2)


def store_packed(target, where, values):
    rows = values.shape[-2]
    full, folded = pack(values)
    target[where + (slice(0, rows),)] = full
    target[where + (slice(rows, rows + rows // 2),)] = folded


STAT, LON, ROW, TOK, MIX, SETUP = range(6)


def rollout(
    lats,
    chans,
    state_hbm,
    gains_hbm,
    shifts_hbm,
    fin_bias_hbm,
    fout_bias_hbm,
    up_bias_hbm,
    fin_hbm,
    fout_hbm,
    up_hbm,
    down_hbm,
    t_lon_hbm,
    t_lat_hbm,
    t_rows_hbm,
    t_back_hbm,
    out_hbm,
    state,
    gains,
    shifts,
    fin_bias,
    fout_bias,
    up_bias,
    x,
    stat_send,
    stat_recv,
    lon_send,
    lon_recv,
    row_send,
    row_recv,
    tok_send,
    tok_recv,
    tok_pair,
    mix_full,
    mix_send,
    mix_pair,
    mix_recv,
    bias_send,
    bias_recv,
    par_send,
    par_recv,
    par,
    fin_raw,
    fout_raw,
    fin,
    fout,
    fin_b,
    fout_b,
    up,
    down,
    up_recv,
    down_recv,
    t_lon,
    t_lat,
    t_rows,
    t_back,
    tokens,
    hidden,
    load_sem,
    send_sem,
    recv_sem,
):
    lat, ch = lax.axis_index("lat"), lax.axis_index("ch")
    core, chip = lax.rem(ch, 2), lax.div(ch, 2)
    chips = chans // 2
    rows, width, _, own = state.shape
    part = x.shape[2]
    near = -(-width // 2)
    wide = chans * own
    hid = up.shape[1]
    spread_modes = t_lon.shape[1]

    def chan(q):
        return 2 * lax.rem(chip + q // 2, chips) + (core if q % 2 == 0 else 1 - core)

    def half_of(q):
        return core if q % 2 == 0 else 1 - core

    others = [2 * lax.rem(chip + j, chips) + n for j in range(1, chips) for n in range(2)]

    def slot_rows(order):
        rest = own - LANES
        pairs = []
        for n, c in enumerate(order):
            first = pl.multiple_of(c * own, rest)
            then = pl.multiple_of(c * own + LANES, rest)
            pairs.append((pl.ds(first, LANES), pl.ds(n * LANES, LANES)))
            pairs.append((pl.ds(then, rest), pl.ds(chans * LANES + n * rest, rest)))
        return pairs

    order = [ch, chan(1)] + others
    up_rows = slot_rows(order)
    partner_rows = slot_rows([chan(1), ch] + others)

    lat_order = sorted(range(1, lats), key=lambda k: -4 * (2 * k // lats) - 2 * (k % 2) - k / lats)
    ch_order = tuple(range(2, chans)) + (1,)

    loads = [
        pltpu.make_async_copy(source, target, load_sem.at[n])
        for n, (source, target) in enumerate(
            (
                (state_hbm, state),
                (gains_hbm, gains),
                (shifts_hbm, shifts),
                (up_bias_hbm, up_bias),
                (fin_bias_hbm, fin_bias),
                (fout_bias_hbm, fout_bias),
                (fin_hbm, fin_raw),
                (fout_hbm, fout_raw),
                (t_lon_hbm, t_lon),
                (t_lat_hbm, t_lat),
                (t_rows_hbm, t_rows),
                (t_back_hbm, t_back),
                (down_hbm, down),
            )
            + tuple((up_hbm.at[source], up.at[target]) for source, target in up_rows)
        )
    ]
    for each in loads:
        each.start()
    stores = [
        pltpu.make_async_copy(state.at[r], out_hbm.at[r], load_sem.at[r]) for r in range(rows)
    ]

    barrier = pltpu.get_barrier_semaphore()
    for k in lat_order:
        pl.semaphore_signal(barrier, inc=1, device_id={"lat": flip(lat, k)}, device_id_type=MESH)
    for q in ch_order:
        pl.semaphore_signal(barrier, inc=1, device_id={"ch": chan(q)}, device_id_type=MESH)

    def copy(kind, r, k, source, target, device):
        return pltpu.make_async_remote_copy(
            src_ref=source,
            dst_ref=target,
            send_sem=send_sem.at[kind, r, k],
            recv_sem=recv_sem.at[kind, r, k],
            device_id=device,
            device_id_type=MESH,
        )

    def stat_copies(r):
        return [
            copy(STAT, r, q, stat_send.at[r], stat_recv.at[r, ch], {"ch": chan(q)})
            for q in ch_order
        ]

    def lon_copies(r):
        return [
            copy(LON, r, k, lon_send.at[r, flip(lat, k)], lon_recv.at[lat, r], {"lat": flip(lat, k)})
            for k in lat_order
        ]

    def row_copies(r):
        return [
            copy(ROW, r, k, row_send.at[r, flip(lat, k)], row_recv.at[r, lat], {"lat": flip(lat, k)})
            for k in lat_order
        ]

    def tok_copies(r):
        copies = []
        for q in range(2, chans):
            slot = 2 * ((chips - q // 2) % chips - 1) + core
            source = tok_send.at[r, half_of(q)]
            copies.append(copy(TOK, r, q, source, tok_recv.at[r, slot], {"ch": chan(q)}))
        copies.append(copy(TOK, r, 1, x.at[r, 1 - core], tok_pair.at[r], {"ch": chan(1)}))
        return copies

    def mix_copy(r, q):
        if q == 1:
            return copy(MIX, r, q, mix_full.at[r, 1 - core], mix_pair.at[r], {"ch": chan(q)})
        n = q // 2 - 1
        source = mix_send.at[r, n, half_of(q)]
        return copy(MIX, r, q, source, mix_recv.at[r, n, core], {"ch": chan(q)})

    def mix_copies(r):
        return [mix_copy(r, q) for q in ch_order]

    def start(copies):
        for each in copies:
            each.start()

    def finish(copies):
        for each in copies:
            each.wait()

    x[...] = jnp.zeros_like(x)
    loads[0].wait()
    for r in range(rows):
        x[r, 0, 0:near] = state[r, 0:near, 0]
        x[r, 1, 0 : width - near] = state[r, near:width, 0]
    ones = jnp.ones((8, own), BF16)
    which = lax.broadcasted_iota(jnp.int32, (8, 2 * part), 0)

    def row_sums(values):
        dims = (((1,), (1,)), ((), ()))
        high, low = halves(values)
        return lax.dot_general(
            ones, high, dims, preferred_element_type=F32
        ) + lax.dot_general(ones, low, dims, preferred_element_type=F32)

    def own_stats(r):
        values = x[r].reshape(2 * part, own)
        sums = jnp.where(which == 0, row_sums(values), row_sums(values * values))
        stat_send[r] = sums[0:2]
        stat_recv[r, pl.ds(ch, 1)] = sums[None, 0:2]

    def take_stats(r):
        with jax.named_scope("wait_stat"):
            finish(stat_copies(r))
        total = stat_recv[r, 0]
        for c in range(1, chans):
            total = total + stat_recv[r, c]
        mean = total[0:1] / wide
        scaled = lax.rsqrt(total[1:2] / wide - mean * mean + EPS)
        both = jnp.transpose(jnp.where(which == 0, mean, scaled))
        return both[:, 0:1], both[:, 1:2]

    for r in range(rows):
        own_stats(r)
    pl.semaphore_wait(barrier, lats + chans - 2)
    for r in range(rows):
        start(stat_copies(r))
    for each in loads[1:4]:
        each.wait()
    gain = gains[...].astype(F32)
    shift = shifts[...].astype(F32)
    par_send[...] = jnp.concatenate((gain[1:2], shift[1:2], jnp.zeros((6, own), F32)), 0)
    par_recv[pl.ds(ch, 1)] = par_send[...][None]
    bias_send[...] = jnp.broadcast_to(up_bias[...].astype(F32)[None], bias_send.shape)
    partner = {"ch": chan(1)}
    setup = [
        copy(SETUP, 0, 0, down_hbm, down_recv, partner),
        copy(SETUP, 0, 1, bias_send, bias_recv, partner),
    ]
    for n, (source, target) in enumerate(partner_rows):
        setup.append(
            copy(SETUP, 1 + n // chans, n % chans, up_hbm.at[source], up_recv.at[target], partner)
        )
    for n, q in enumerate(ch_order):
        setup.append(copy(SETUP, 0, 2 + n, par_send, par_recv.at[ch], {"ch": chan(q)}))
    start(setup)
    for each in loads[4:8]:
        each.wait()
    blocks, size = fin_raw.shape[1], fin_raw.shape[2]
    line = lax.broadcasted_iota(jnp.int32, (size, own), 0)
    lane = lax.broadcasted_iota(jnp.int32, (size, own), 1)
    for raw, target, bias, bias_target in (
        (fin_raw, fin, fin_bias, fin_b),
        (fout_raw, fout, fout_bias, fout_b),
    ):
        placed = 0.0
        for n in range(blocks):
            shifted = jnp.where(lane == line + n * size, 1.0, 0.0)
            select = shifted.astype(BF16)
            for p in range(2):
                high, low = halves(raw[p, n])
                target[p, 0, n * size : (n + 1) * size] = dot(high, select).astype(BF16)
                target[p, 1, n * size : (n + 1) * size] = dot(low, select).astype(BF16)
            placed = placed + jnp.dot(
                bias[:, n, :], shifted, precision=HIGH, preferred_element_type=F32
            )
        bias_target[...] = placed
    for each in loads[8:12]:
        each.wait()

    def complex_apply(pair, weights, bias):
        split = pair.shape[0] // 2
        pair = halves(pair)
        one = dot3(pair, (weights[0, 0], weights[0, 1]))
        two = dot3(pair, (weights[1, 0], weights[1, 1]))
        return (
            one[:split] - two[split:] + bias[0:1, :],
            one[split:] + two[:split] + bias[1:2, :],
        )

    def spectrum(messages, count):
        full = messages[..., :count, :]
        rest = unfold(messages[..., count:, :]).astype(BF16)
        return jnp.concatenate((full, rest), -1).reshape(-1, own)

    share = spread_modes // lats

    def forward(r):
        with jax.named_scope("forward"):
            mean, scaled = take_stats(r)
            now = x[r].reshape(2 * part, own)
            normed = (now - mean) * scaled * gain[0:1] + shift[0:1]
            x[r] = (now + normed).reshape(2, part, own)
            spectra = dot3((t_lon[0], t_lon[1]), halves(normed))
            store_packed(lon_send, (r, slice(None)), spectra.reshape(lats, share, own))
            start(lon_copies(r))
            lon_recv[pl.ds(lat, 1), r] = lon_send[r, pl.ds(lat, 1)]

    def spectral():
        data = spectrum(lon_recv[...], share)
        size = t_lat.shape[1] // 4
        spec = []
        for n in range(4):
            cut = slice(n * size, (n + 1) * size)
            spec.append(dot(t_lat[0, cut], data) + dot(t_lat[1, cut], data))
        spec = jnp.concatenate(spec, 0)
        real, imag = complex_apply(spec, fin, fin_b)
        pair = jnp.concatenate((jnp.maximum(real, 0.0), jnp.maximum(imag, 0.0)), 0)
        real, imag = complex_apply(pair, fout, fout_b)
        return halves(jnp.concatenate((soft_shrink(real), soft_shrink(imag)), 0))

    def unmix(r, pair):
        count = spread_modes // 2
        for n in range(2):
            first = r * spread_modes + n * count
            cut = slice(first, first + count)
            back = dot3((t_rows[0, cut], t_rows[1, cut]), pair)
            where = (r, slice(n * lats // 2, (n + 1) * lats // 2))
            store_packed(row_send, where, back.reshape(lats // 2, share, own))
        start(row_copies(r))
        row_recv[r, pl.ds(lat, 1)] = row_send[r, pl.ds(lat, 1)]

    def backward(r):
        data = spectrum(row_recv[r], share)
        back = dot(t_back[0], data) + dot(t_back[1], data)
        now = x[r] + back.reshape(2, part, own)
        x[r] = now
        store_packed(tok_send, (r, slice(None)), now)
        start(tok_copies(r))

    def token_piece(r, n):
        if n == 0:
            return x[r, pl.ds(core, 1), :, :LANES][0]
        if n == 1:
            return tok_pair[r, :, :LANES]
        if n == chans:
            mine = x[r, pl.ds(core, 1), :, LANES:][0]
            return jnp.concatenate((mine, tok_pair[r, :, LANES:]), -1)
        if n < chans:
            return tok_recv[r, n - 2, 0:part].astype(F32)
        c = 2 * (n - chans - 1)
        one = tok_recv[r, c, part : part + part // 2].astype(F32)
        two = tok_recv[r, c + 1, part : part + part // 2].astype(F32)
        rest = LANES // 2
        upper = jnp.concatenate((one[:, :rest], two[:, :rest]), -1)
        lower = jnp.concatenate((one[:, rest:], two[:, rest:]), -1)
        return jnp.concatenate((upper, lower), 0)

    def normalize(r):
        total, squares = 0.0, 0.0
        for n in range(wide // LANES):
            piece = token_piece(r, n)
            total = total + piece
            squares = squares + piece * piece
        mean = jnp.sum(total, -1, keepdims=True) / wide
        spread = jnp.sum(squares, -1, keepdims=True) / wide - mean * mean
        scaled = lax.rsqrt(spread + EPS)
        for n in range(wide // LANES):
            cut = slice(n * LANES, (n + 1) * LANES)
            normed = (token_piece(r, n) - mean) * scaled * par[0:1, cut] + par[1:2, cut]
            high, low = halves(normed)
            tokens[r % 2, 0:part, cut] = high
            near = n in (0, 1, chans)
            tokens[r % 2, part : 2 * part, cut] = jnp.zeros_like(low) if near else low

    def project_up(r):
        for s, (weight, bias) in enumerate(((up, bias_send), (up_recv, bias_recv))):
            for lo in range(0, hid, 256):
                cut = slice(lo, lo + 256)
                both = dot(tokens[r % 2], weight[:, cut])
                pre = both[:part] + both[part:] + bias[0:1, cut]
                hidden[s, :, cut] = gelu(pre).astype(BF16)

    def project_down(r):
        for j in tuple(range(1, chips)) + (0,):
            first = pl.multiple_of(2 * own * lax.rem(chip + j, chips), LANES)
            cut = pl.ds(first, 2 * own)
            mixed = dot(hidden[0], down[:, cut]) + dot(hidden[1], down_recv[:, cut])
            for n in range(2):
                piece = mixed[:, n * own : (n + 1) * own]
                if j:
                    store_packed(mix_send, (r, j - 1, n), piece)
                else:
                    mix_full[r, n] = piece
            for q in (2 * j, 2 * j + 1):
                if q:
                    mix_copy(r, q).start()

    def residual(r):
        for h, piece in ((core, mix_full[r, pl.ds(core, 1)]), (1 - core, mix_pair[r][None])):
            for n in range(chips - 1):
                message = mix_recv[r, n, pl.ds(h, 1)]
                rest = unfold(message[:, part:])
                piece = piece + jnp.concatenate((message[:, :part].astype(F32), rest), -1)
            x[r, pl.ds(h, 1)] = x[r, pl.ds(h, 1)] + piece + shift[2:3]

    @pl.loop(0, STEPS)
    def _(index):
        for r in range(rows):
            forward(r)
        with jax.named_scope("wait_lon"):
            for r in range(rows):
                finish(lon_copies(r))
        with jax.named_scope("spectral"):
            pair = spectral()
        with jax.named_scope("unmix"):
            for r in range(rows):
                unmix(r, pair)
        for r in range(rows):
            with jax.named_scope("wait_row"):
                finish(row_copies(r))
            with jax.named_scope("backward"):
                backward(r)

        @pl.when(index == 0)
        def _():
            for each in loads[12:]:
                each.wait()
            finish(setup)
            pieces = [par_recv[c, 0:2, :LANES] for c in order]
            pieces += [par_recv[c, 0:2, LANES:] for c in order]
            par[...] = jnp.concatenate(pieces, -1)

        for r in range(rows):
            if r <= 1:
                with jax.named_scope("wait_tok"):
                    finish(tok_copies(r))
                with jax.named_scope("norm"):
                    normalize(r)
            with jax.named_scope("up"):
                project_up(r)
            if 1 <= r < rows - 1:
                with jax.named_scope("wait_tok"):
                    finish(tok_copies(r + 1))
            with jax.named_scope("down"):
                if 1 <= r < rows - 1:
                    normalize(r + 1)
                project_down(r)
        for r in range(rows):
            with jax.named_scope("wait_mix"):
                finish(mix_copies(r))
            with jax.named_scope("residual"):
                residual(r)

            @pl.when(index == STEPS - 1)
            def _():
                state[r, 0:near, 0] = x[r, 0, 0:near]
                state[r, near:width, 0] = x[r, 1, 0 : width - near]
                stores[r].start()

            @pl.when(index < STEPS - 1)
            def _():
                own_stats(r)
                start(stat_copies(r))

    for each in stores:
        each.wait()


def hand_over(source, target, held, read_sem, write_sem):
    rows = source.shape[0]
    reads = [pltpu.make_async_copy(source.at[r], held.at[r], read_sem.at[r]) for r in range(rows)]
    writes = [pltpu.make_async_copy(held.at[r], target.at[r], write_sem.at[r]) for r in range(rows)]
    for each in reads:
        each.start()
    for read, write in zip(reads, writes):
        read.wait()
        write.start()
    for each in writes:
        each.wait()


def fused(
    lats,
    chans,
    state,
    norm_gains,
    channel_biases,
    filter_in,
    filter_in_bias,
    filter_out,
    filter_out_bias,
    up_weight,
    up_bias,
    down_weight,
):
    _, rows, width, own = state.shape
    part = -(--(-width // 2) // 16) * 16
    share = 2 * M // lats
    hid = up_weight.shape[1]
    tables = tuple(
        jnp.asarray(t) for t in fourier_tables(width, part, rows * lats, M, lats)
    )
    args = (
        state.transpose(1, 2, 0, 3),
        norm_gains,
        channel_biases,
        filter_in_bias,
        filter_out_bias,
        up_bias,
        filter_in,
        filter_out,
        up_weight,
        down_weight,
    ) + tables
    hbm = pl.BlockSpec(memory_space=pltpu.HBM)
    packed = share + share // 2
    spectrum = (rows, lats, packed, LANES)
    folded = part + part // 2
    peers = max(lats, chans)
    result = pl.pallas_call(
        functools.partial(rollout, lats, chans),
        out_shape=jax.ShapeDtypeStruct((rows, width, 1, own), F32),
        in_specs=[hbm] * 14,
        out_specs=hbm,
        scratch_shapes=[
            pltpu.VMEM((rows, width, 1, own), F32),
            pltpu.VMEM(norm_gains.shape, BF16),
            pltpu.VMEM(channel_biases.shape, BF16),
            pltpu.VMEM(filter_in_bias.shape, F32),
            pltpu.VMEM(filter_out_bias.shape, F32),
            pltpu.VMEM(up_bias.shape, BF16),
            pltpu.VMEM((rows, 2, part, own), F32),
            pltpu.VMEM((rows, 2, 2 * part), F32),
            pltpu.VMEM((rows, chans, 2, 2 * part), F32),
            pltpu.VMEM(spectrum, BF16),
            pltpu.VMEM((lats, rows, packed, LANES), BF16),
            pltpu.VMEM(spectrum, BF16),
            pltpu.VMEM(spectrum, BF16),
            pltpu.VMEM((rows, 2, folded, LANES), BF16),
            pltpu.VMEM((rows, chans - 2, folded, LANES), BF16),
            pltpu.VMEM((rows, part, own), F32),
            pltpu.VMEM((rows, 2, part, own), F32),
            pltpu.VMEM((rows, chans // 2 - 1, 2, folded, LANES), BF16),
            pltpu.VMEM((rows, part, own), F32),
            pltpu.VMEM((rows, chans // 2 - 1, 2, folded, LANES), BF16),
            pltpu.VMEM((8, hid), F32),
            pltpu.VMEM((8, hid), F32),
            pltpu.VMEM((8, own), F32),
            pltpu.VMEM((chans, 8, own), F32),
            pltpu.VMEM((2, chans * own), F32),
            pltpu.VMEM(filter_in.shape, F32),
            pltpu.VMEM(filter_out.shape, F32),
            pltpu.VMEM((2, 2, own, own), BF16),
            pltpu.VMEM((2, 2, own, own), BF16),
            pltpu.VMEM((2, own), F32),
            pltpu.VMEM((2, own), F32),
            pltpu.VMEM(up_weight.shape, BF16),
            pltpu.VMEM(down_weight.shape, BF16),
            pltpu.VMEM(up_weight.shape, BF16),
            pltpu.VMEM(down_weight.shape, BF16),
        ]
        + [pltpu.VMEM(t.shape, BF16) for t in tables]
        + [
            pltpu.VMEM((2, 2 * part, chans * own), BF16),
            pltpu.VMEM((2, part, hid), BF16),
            pltpu.SemaphoreType.DMA((13 + 2 * chans,)),
            pltpu.SemaphoreType.DMA((6, max(rows, 3), peers)),
            pltpu.SemaphoreType.DMA((6, max(rows, 3), peers)),
        ],
        compiler_params=pltpu.CompilerParams(
            collective_id=0, has_side_effects=True, vmem_limit_bytes=60 * 1024 * 1024
        ),
    )(*args)
    result = pl.pallas_call(
        hand_over,
        out_shape=jax.ShapeDtypeStruct(result.shape, F32),
        in_specs=[hbm],
        out_specs=hbm,
        scratch_shapes=[
            pltpu.VMEM(result.shape, F32),
            pltpu.SemaphoreType.DMA((rows,)),
            pltpu.SemaphoreType.DMA((rows,)),
        ],
        compiler_params=pltpu.CompilerParams(vmem_limit_bytes=60 * 1024 * 1024),
    )(result)
    return result.transpose(2, 0, 1, 3)


def dispatch(sizes, *args):
    lats, chans = sizes["lat"], sizes["ch"]
    own = args[0].shape[3]
    folds = own // LANES == 1 and 2 * (own % LANES) == LANES
    if folds and 2 * M // lats % 16 == 0 and chans > 2 and chans % 2 == 0:
        return fused(lats, chans, *args)
    return local(*args)


def solution(mesh):
    placed = (
        P(None, "lat", None, "ch"),
        P(None, "ch"),
        P(None, "ch"),
        P(None, "ch", None, None),
        P(None, "ch", None),
        P(None, "ch", None, None),
        P(None, "ch", None),
        P(None, "ch"),
        P("ch"),
        P("ch", None),
    )
    return jax.shard_map(
        functools.partial(dispatch, dict(mesh.shape)), mesh=mesh, in_specs=placed, out_specs=P(None, "lat", None, "ch"), check_vma=False
    )
```
